128 devices in a mesh: span: 32 (over y, z, core), wall: 4 (over x).
Axes of the slice: x: 4, y: 4, z: 4, core: 2. Of those that a mesh axis runs over, the one named last changes fastest.
Arguments:
- random_field: float32 [3, 2048, 65536], P(None, 'wall', 'span'), may hold values from -6 to 6
- half_widths: int32 [2048], replicated, may hold values from 1 to 256, as said below
- band_pads: int32 [32], replicated, may hold values from 1 to 256, as said below
- span_widths: int32 [32], replicated, may hold values from 1 to 64, as said below
- stresses: float32 [6, 2048], P(None, 'wall'), as said below
- mean_flow: float32 [2048], P('wall'), may hold values from 0.3 to 1.2
Outputs:
- velocity: float32 [3, 2048, 65536], P(None, 'wall', 'span')
The draws below stay inside these ranges and needn't reach their ends.
Inputs may be any that keep to these rules, and one draw needn't show every extreme that they name: `half_widths`: every row's value is at most the band_pads value of its band of 64 rows; some row reaches 256. `band_pads`: some band reaches 256. `span_widths`: some band reaches 64. `stresses`: each row's six entries form a positive definite tensor whose correlation coefficients are at most 0.4 in magnitude; the diagonal entries lie between 0.3 and 3.
All inputs are finite; a program needn't handle non-finite values.
Results may differ from the reference program's by a relative error of at most 0.0003.
Values sent between devices are 32-bit elements; how exact they have to be, the bound alone decides.
No kernel may reach another device: no remote copies, remote signals or barrier semaphores. Data moves between devices by JAX's collectives and lax.ppermute only.
A program may use at most 192 MiB of HBM per device.

```python
import jax
import jax.numpy as jnp
from jax import lax

MAXW = 256
SPMAX = 64
BAND = 64
NY = 2048
NS = 65536


def wall_tables(key):
    base = jax.random.fold_in(key, 4711)
    first, second, third = jax.random.split(base, 3)
    band_total = NY // BAND
    band_pads = jax.random.randint(first, (band_total,), 1, MAXW + 1)
    chosen = jax.random.randint(second, (), 0, band_total)
    band_pads = jnp.where(jnp.arange(band_total) == chosen, MAXW, band_pads)
    raw_draw = jax.random.randint(third, (band_total * BAND,), 0, MAXW)
    halves = 1 + raw_draw % jnp.repeat(band_pads, BAND)
    halves = jnp.where(jnp.arange(band_total * BAND) == chosen * BAND, MAXW, halves)
    return (band_pads.astype(jnp.int32), halves.astype(jnp.int32))


def draw_half_widths(key, part):
    return wall_tables(key)[1]


def draw_band_pads(key, part):
    return wall_tables(key)[0]


def draw_span_widths(key, part):
    base = jax.random.fold_in(key, 919)
    first, second = jax.random.split(base)
    band_total = NY // BAND
    widths = jax.random.randint(first, (band_total,), 1, SPMAX + 1)
    chosen = jax.random.randint(second, (), 0, band_total)
    return jnp.where(jnp.arange(band_total) == chosen, SPMAX, widths).astype(jnp.int32)


def draw_stresses(key, part):
    base = jax.random.fold_in(key, 313)
    first, second = jax.random.split(base)
    logs = jax.random.uniform(first, (3, NY), jnp.float32, jnp.log(0.3), jnp.log(3.0))
    diagonal = jnp.exp(logs)
    correl = jax.random.uniform(second, (3, NY), jnp.float32, -0.4, 0.4)
    cross_uv = correl[0] * jnp.sqrt(diagonal[0] * diagonal[1])
    cross_uw = correl[1] * jnp.sqrt(diagonal[0] * diagonal[2])
    cross_vw = correl[2] * jnp.sqrt(diagonal[1] * diagonal[2])
    return jnp.stack([diagonal[0], diagonal[1], diagonal[2], cross_uv, cross_uw, cross_vw], axis=0).astype(jnp.float32)


def levels(rng, dims, pieces, least, top_value):
    level, own = 1.0, jax.random.fold_in(rng, 6)
    for position, shards_of in pieces:
        draws = jnp.exp(jax.random.uniform(jax.random.fold_in(own, position), (shards_of,), jnp.float32, least / len(pieces), top_value / len(pieces)))
        level = level * jnp.repeat(draws, dims[position] // shards_of).reshape([-1 if axis == position else 1 for axis in range(len(dims))])
    return level


def noise(rng, shape, scale, limit, cuts=(), held_as=jnp.bfloat16):
    factor_of = levels(rng, shape, cuts, -0.22, 0.18) if cuts else 1.0
    array = jax.random.normal(rng, shape, jnp.float32) * scale * factor_of
    return jnp.minimum(jnp.maximum(array, -limit), limit).astype(held_as)


def setup_inputs(seed: int = 0) -> dict:
    keys = jax.random.split(jax.random.key(seed), 7)
    return {
        "random_field": noise(keys[0], (3, NY, NS), 1.0, 6.0, ((1, 4), (2, 32)), jnp.float32),
        "half_widths": draw_half_widths(jax.random.fold_in(keys[6], 71), 0),
        "band_pads": draw_band_pads(jax.random.fold_in(keys[6], 71), 0),
        "span_widths": draw_span_widths(jax.random.fold_in(keys[6], 71), 0),
        "stresses": draw_stresses(jax.random.fold_in(keys[6], 71), 0),
        "mean_flow": jnp.clip(0.3 + 0.90000004 * jax.random.uniform(keys[5], (NY,), jnp.float32) ** levels(keys[5], (NY,), ((0, 4),), -0.2, 0.2), 0.3, 1.2),
    }


def wall_kernel(halves, pad_value):
    offsets = (jnp.arange(BAND + 2 * MAXW)[None, :] - MAXW - jnp.arange(BAND)[:, None]).astype(jnp.float32)
    spread = halves.astype(jnp.float32)[:, None]
    inside = jnp.abs(offsets) <= pad_value.astype(jnp.float32)
    coeffs = jnp.where(inside, jnp.exp(-jnp.pi * offsets * offsets / (2.0 * spread * spread)), jnp.float32(0.0))
    return coeffs / jnp.sqrt(lax.optimization_barrier(jnp.sum(coeffs * coeffs, axis=1, keepdims=True)))

def lund_apply(psi, stresses, mean_flow):
    lund_aa = jnp.sqrt(stresses[0])
    lund_ba = stresses[3] / lund_aa
    lund_bb = jnp.sqrt(stresses[1] - lund_ba * lund_ba)
    lund_ca = stresses[4] / lund_aa
    lund_cb = (stresses[5] - lund_ba * lund_ca) / lund_bb
    lund_cc = jnp.sqrt(stresses[2] - lund_ca * lund_ca - lund_cb * lund_cb)
    stream = mean_flow[:, None] + lund_aa[:, None] * psi[0]
    normal = lund_ba[:, None] * psi[0] + lund_bb[:, None] * psi[1]
    spanwise = lund_ca[:, None] * psi[0] + lund_cb[:, None] * psi[1] + lund_cc[:, None] * psi[2]
    return jnp.stack([stream, normal, spanwise], axis=0)

def reference(random_field, half_widths, band_pads, span_widths, stresses, mean_flow):
    channels, total_rows, total_cols = random_field.shape
    reach = 2 * SPMAX
    wrapped = jnp.concatenate([random_field[:, :, total_cols - reach:], random_field, random_field[:, :, :reach]], axis=2)
    row_widths = jnp.repeat(span_widths, BAND).astype(jnp.float32)
    offsets = (jnp.arange(2 * reach + 1) - reach).astype(jnp.float32)
    profile = jnp.where(jnp.abs(offsets)[:, None] <= 2.0 * row_widths[None, :], jnp.exp(-jnp.pi * offsets[:, None] ** 2 / (2.0 * row_widths[None, :] ** 2)), jnp.float32(0.0))
    profile = profile / jnp.sqrt(lax.optimization_barrier(jnp.sum(profile * profile, axis=0, keepdims=True)))

    def accumulate(shift_index, total):
        shift_index = jnp.asarray(shift_index).astype(jnp.int32)
        piece = lax.dynamic_slice_in_dim(wrapped, shift_index, total_cols, 2)
        weight = lax.dynamic_index_in_dim(profile, shift_index, 0, keepdims=False)
        return total + weight[None, :, None] * piece
    spanwise = lax.fori_loop(0, 2 * reach + 1, accumulate, jnp.zeros(random_field.shape, jnp.float32))
    extended = jnp.pad(spanwise, ((0, 0), (MAXW, MAXW), (0, 0)))

    def one_band(band_index):
        start = (band_index * BAND).astype(jnp.int32)
        window = lax.dynamic_slice_in_dim(extended, start, BAND + 2 * MAXW, 1)
        halves = lax.dynamic_slice_in_dim(half_widths, start, BAND, 0)
        pad_value = lax.dynamic_index_in_dim(band_pads, band_index.astype(jnp.int32), 0, keepdims=False)
        kernel = wall_kernel(halves, pad_value)
        return jnp.einsum('ij,cjs->cis', kernel, window, precision=lax.Precision.HIGHEST)
    blocks = lax.map(one_band, jnp.arange(total_rows // BAND).astype(jnp.int32))
    psi = jnp.moveaxis(blocks, 0, 1).reshape(channels, total_rows, total_cols)
    return lund_apply(psi, stresses, mean_flow)
```

```python
import functools

import jax
import jax.numpy as jnp
from jax import lax
from jax.experimental import pallas as pl
from jax.experimental.pallas import tpu as pltpu
from jax.sharding import PartitionSpec as P

MAXW = 256
SPMAX = 64
BAND = 64
REACH = 2 * SPMAX
TILE = 4 * SPMAX
SIZES = (256,)


def halves_of(values):
    high = lax.reduce_precision(values, 8, 7)
    return high.astype(jnp.bfloat16), (values - high).astype(jnp.bfloat16)


def split(values):
    high = values.astype(jnp.bfloat16)
    return high, (values - high.astype(jnp.float32)).astype(jnp.bfloat16)


def dot(left, right):
    return lax.dot_general(left, right, (((1,), (0,)), ((), ())), preferred_element_type=jnp.float32)


def dot3(left_high, left_low, right_high, right_low):
    return dot(left_high, right_high) + (dot(left_high, right_low) + dot(left_low, right_high))


def span_tables(span_here):
    spread = span_here.astype(jnp.float32)
    offsets = jnp.arange(-REACH, REACH + 1).astype(jnp.float32)
    profile = jnp.where(
        jnp.abs(offsets)[None, :] <= 2.0 * spread[:, None],
        jnp.exp(-jnp.pi * offsets[None, :] ** 2 / (2.0 * spread[:, None] ** 2)),
        0.0,
    )
    scale = 1.0 / jnp.sqrt(jnp.sum(profile * profile, axis=1))
    shifts = (jnp.arange(2 * TILE)[:, None] - REACH - jnp.arange(TILE)[None, :]).astype(jnp.float32)
    wide = spread[:, None, None]
    coeffs = jnp.where(
        jnp.abs(shifts)[None] <= 2.0 * wide,
        jnp.exp(shifts[None] * shifts[None] * (-jnp.pi / (2.0 * wide * wide))) * scale[:, None, None],
        0.0,
    )
    return halves_of(coeffs)


def wall_coeff(distance, width, pad, inverse):
    return jnp.where(
        distance <= pad, jnp.exp(distance * distance * (-jnp.pi / (2.0 * width * width))) * inverse, 0.0
    )


def reach_of(half_widths, row_pads):
    return jnp.minimum(row_pads, (half_widths * 41 + 4) // 5)


def cover_cost(need):
    counts = jnp.arange(MAXW + 1)
    return counts[None, :] + jnp.sum((need[:, None, :] > counts[None, :, None]).astype(jnp.int32), axis=2)


def edge_tables(half_widths, row_pads, first_row, rows_here):
    half_pad = jnp.pad(half_widths, (MAXW, MAXW), constant_values=1)
    pad_pad = jnp.pad(row_pads, (MAXW, MAXW), constant_values=1)
    width_w = lax.dynamic_slice_in_dim(half_pad, first_row, rows_here + 2 * MAXW, 0)
    pad_w = lax.dynamic_slice_in_dim(pad_pad, first_row, rows_here + 2 * MAXW, 0)
    steps = jnp.arange(MAXW + 1).astype(jnp.float32)
    width_f = width_w.astype(jnp.float32)
    pad_f = pad_w.astype(jnp.float32)
    half_profile = wall_coeff(steps[None, :], width_f[:, None], pad_f[:, None], 1.0)
    inverse_w = 1.0 / jnp.sqrt(2.0 * jnp.sum(half_profile * half_profile, axis=1) - 1.0)

    def four(values):
        end = rows_here + MAXW
        return jnp.stack(
            [values[MAXW : 2 * MAXW], values[end - MAXW : end], values[:MAXW], values[end : end + MAXW]], axis=0
        )

    width, pad, inverse = four(width_f), four(pad_f), four(inverse_w)
    index = jnp.arange(MAXW)
    depth = jnp.stack([index, MAXW - 1 - index, MAXW - 1 - index, index], axis=0)
    need = four(reach_of(width_w, pad_w)) - depth
    cost = cover_cost(need)
    best = jnp.min(cost * 512 + jnp.arange(MAXW + 1)[None, :], axis=1) % 512
    part = need > best[:, None]
    before = jnp.sum((part[:, None, :] & (index[None, None, :] < index[None, :, None])).astype(jnp.int32), axis=2)
    place = jnp.where(part, best[:, None] + before, -1)
    depth_f = depth.astype(jnp.float32)

    slot = index[None, None, :]
    taken = place[:2, :, None] == slot
    far = (depth[:2, :, None] + slot + 1).astype(jnp.float32)
    plain = wall_coeff(far, width[:2, :, None], pad[:2, :, None], inverse[:2, :, None])
    plain = jnp.where(part[:2, :, None] | (slot >= best[:2, None, None]), 0.0, plain)
    take = jnp.where(taken, 1.0, plain)

    chosen = (place[2:, None, :] == index[None, :, None]).astype(jnp.float32)

    def pick(values):
        return jnp.sum(chosen * values[2:, None, :], axis=2)

    width_q, pad_q, inverse_q, depth_q = pick(width), pick(pad), pick(inverse), pick(depth_f)
    away = jnp.stack([index + 1, MAXW - index], axis=0)
    far_q = depth_q[:, :, None] + away[:, None, :].astype(jnp.float32)
    summed = wall_coeff(far_q, jnp.maximum(width_q, 1.0)[:, :, None], pad_q[:, :, None], inverse_q[:, :, None])
    nearest = (away[:, None, :] == index[None, :, None] + 1).astype(jnp.float32)
    give = jnp.where(index[None, :, None] < best[2:, None, None], nearest, summed)

    inner = slice(MAXW, MAXW + rows_here)
    rows = jnp.arange(rows_here)
    apart = jnp.abs(rows[:, None] - rows[None, :]).astype(jnp.float32)
    local = wall_coeff(apart, width_f[inner, None], pad_f[inner, None], inverse_w[inner, None])
    return halves_of(take), halves_of(give), halves_of(local)


def rows_needed(half_widths, row_pads, rows_here):
    total = half_widths.shape[0]
    reach = reach_of(half_widths, row_pads)
    index = jnp.arange(MAXW)
    needs = []
    for cut in range(rows_here, total, rows_here):
        needs.append(reach[cut : cut + MAXW] - index)
        needs.append(reach[cut - MAXW : cut] - (MAXW - 1 - index))
    return jnp.max(jnp.min(cover_cost(jnp.stack(needs, axis=0)), axis=1))


def lund_columns(stresses, mean_flow):
    lund_aa = jnp.sqrt(stresses[0])
    lund_ba = stresses[3] / lund_aa
    lund_bb = jnp.sqrt(stresses[1] - lund_ba * lund_ba)
    lund_ca = stresses[4] / lund_aa
    lund_cb = (stresses[5] - lund_ba * lund_ca) / lund_bb
    lund_cc = jnp.sqrt(stresses[2] - lund_ca * lund_ca - lund_cb * lund_cb)
    return jnp.stack([lund_aa, lund_ba, lund_bb, lund_ca, lund_cb, lund_cc, mean_flow, mean_flow], axis=1)


def front_kernel(tiles, bands, x_ref, low_ref, high_ref, gh_ref, gl_ref, wh_ref, wl_ref, *rest):
    sh_ref, sl_ref, send_ref = rest[-3:]
    band = pl.program_id(0)
    wide = jnp.concatenate([low_ref[0], x_ref[0], high_ref[0]], axis=1)
    wide_high, wide_low = split(wide)
    x_high = jnp.concatenate([wide_high[:, t * TILE : (t + 2) * TILE] for t in range(tiles)], axis=0)
    x_low = jnp.concatenate([wide_low[:, t * TILE : (t + 2) * TILE] for t in range(tiles)], axis=0)
    high, low = split(dot3(x_high, x_low, gh_ref[0], gl_ref[0]))
    start = pl.multiple_of(band * BAND, BAND)
    for t in range(tiles):
        sh_ref[0, pl.ds(start, BAND), t * TILE : (t + 1) * TILE] = high[t * BAND : (t + 1) * BAND]
        sl_ref[0, pl.ds(start, BAND), t * TILE : (t + 1) * TILE] = low[t * BAND : (t + 1) * BAND]

    @pl.when(band == bands - 1)
    def _():
        step = 2 * TILE
        for t in range(tiles // 2):
            cols = slice(t * step, (t + 1) * step)
            send_ref[:, cols] = dot3(wh_ref[...], wl_ref[...], sh_ref[0, :, cols], sl_ref[0, :, cols])


def front(field, low, high, tables, give, held, channel, halo_channel, half):
    channels, rows, cols = field.shape
    bands = MAXW // BAND
    tiles = cols // TILE
    size = give[0].shape[0]
    first = half * (rows // BAND - bands)
    first_block = half * (rows // MAXW - 1)
    full = lambda b: (0, 0)
    row_block = lambda c, b: (c, first + b, 0)
    in_specs = [
        pl.BlockSpec((1, BAND, cols), lambda b: row_block(channel, b)),
        pl.BlockSpec((1, BAND, REACH), lambda b: row_block(halo_channel, b)),
        pl.BlockSpec((1, BAND, REACH), lambda b: row_block(halo_channel, b)),
        pl.BlockSpec((1, 2 * TILE, TILE), lambda b: (first + b, 0, 0)),
        pl.BlockSpec((1, 2 * TILE, TILE), lambda b: (first + b, 0, 0)),
        pl.BlockSpec((size, MAXW), full),
        pl.BlockSpec((size, MAXW), full),
    ]
    operands = [field, low, high, *tables, *give]
    aliases = {}
    if held is not None:
        in_specs += [pl.BlockSpec(memory_space=pl.ANY)] * 2
        aliases = {len(operands): 0, len(operands) + 1: 1}
        operands += list(held)
    kept = jax.ShapeDtypeStruct((channels, rows, cols), jnp.bfloat16)
    kept_spec = pl.BlockSpec((1, MAXW, cols), lambda b: (channel, first_block, 0))
    return pl.pallas_call(
        functools.partial(front_kernel, tiles, bands),
        grid=(bands,),
        in_specs=in_specs,
        out_specs=[kept_spec, kept_spec, pl.BlockSpec((size, cols), full)],
        out_shape=[kept, kept, jax.ShapeDtypeStruct((size, cols), jnp.float32)],
        input_output_aliases=aliases,
        cost_estimate=pl.CostEstimate(
            flops=6 * MAXW * cols * 2 * TILE + 6 * size * MAXW * cols,
            bytes_accessed=MAXW * cols * 8 + size * cols * 4,
            transcendentals=0,
        ),
        name="front",
    )(*operands)


def local_kernel(sh_ref, sl_ref, hh_ref, hl_ref, lund_ref, out_ref):
    lund = lund_ref[...]
    column = lambda k: lund[:, k : k + 1]
    psi = dot3(hh_ref[...], hl_ref[...], sh_ref[0], sl_ref[0])
    out_ref[0] = column(6) + column(0) * psi
    normal = column(1) * psi
    spanwise = column(3) * psi
    psi = dot3(hh_ref[...], hl_ref[...], sh_ref[1], sl_ref[1])
    out_ref[1] = normal + column(2) * psi
    spanwise = spanwise + column(4) * psi
    psi = dot3(hh_ref[...], hl_ref[...], sh_ref[2], sl_ref[2])
    out_ref[2] = spanwise + column(5) * psi


def local_filter(held, local, lund):
    channels, rows, cols = held[0].shape
    step = TILE
    block = pl.BlockSpec((channels, rows, step), lambda t: (0, 0, t))
    full = lambda t: (0, 0)
    return pl.pallas_call(
        local_kernel,
        grid=(cols // step,),
        in_specs=[
            block,
            block,
            pl.BlockSpec((rows, rows), full),
            pl.BlockSpec((rows, rows), full),
            pl.BlockSpec((rows, lund.shape[1]), full),
        ],
        out_specs=block,
        out_shape=jax.ShapeDtypeStruct((channels, rows, cols), jnp.float32),
        cost_estimate=pl.CostEstimate(
            flops=6 * channels * rows * rows * cols, bytes_accessed=channels * rows * cols * 8, transcendentals=0
        ),
        name="local",
    )(*held, *local, lund)


def correct_kernel(channel, recv_ref, ah_ref, al_ref, lund_ref, out_in_ref, out_ref, sum_ref):
    target = pl.program_id(1)
    last = 2

    def contribution():
        high, low = split(recv_ref[...])
        return dot3(ah_ref[...], al_ref[...], high, low)

    for k in range(last + 1 - channel):
        row = channel + k
        column = row * (row + 1) // 2 + channel

        @pl.when(target == k)
        def _(k=k, column=column):
            value = contribution() if k == 0 else sum_ref[...]
            if k == 0 and channel < last:
                sum_ref[...] = value
            out_ref[0] = out_in_ref[0] + lund_ref[:, column : column + 1] * value


def correct(out, recv, take, lund, channel, half):
    channels, rows, cols = out.shape
    size = recv.shape[0]
    step = 4 * TILE if channel == channels - 1 else 2 * TILE
    block_row = half * (rows // MAXW - 1)
    block = pl.BlockSpec((1, MAXW, step), lambda t, k: (channel + k, block_row, t))
    full = lambda t, k: (0, 0)
    return pl.pallas_call(
        functools.partial(correct_kernel, channel),
        grid=(cols // step, channels - channel),
        in_specs=[
            pl.BlockSpec((size, step), lambda t, k: (0, t)),
            pl.BlockSpec((MAXW, size), full),
            pl.BlockSpec((MAXW, size), full),
            pl.BlockSpec((MAXW, lund.shape[1]), lambda t, k: (block_row, 0)),
            block,
        ],
        out_specs=block,
        out_shape=jax.ShapeDtypeStruct(out.shape, out.dtype),
        scratch_shapes=[pltpu.VMEM((MAXW, step), jnp.float32)],
        input_output_aliases={4: 0},
        cost_estimate=pl.CostEstimate(
            flops=6 * MAXW * size * cols,
            bytes_accessed=(channels - channel) * MAXW * cols * 8 + size * cols * 4,
            transcendentals=0,
        ),
        name="correct",
    )(recv, *take, lund, out)


def exchange(field, channels):
    count = lax.axis_size("span")
    forward = [(i, (i + 1) % count) for i in range(count)]
    backward = [(target, source) for source, target in forward]
    part = field[channels]
    low = lax.ppermute(part[:, :, -REACH:], "span", forward)
    high = lax.ppermute(part[:, :, :REACH], "span", backward)
    return low, high


def shards(random_field, half_widths, band_pads, span_widths, stresses, mean_flow):
    channels, rows_here, _ = random_field.shape
    wall_count = lax.axis_size("wall")
    first_row = lax.axis_index("wall") * rows_here
    halos = [exchange(random_field, slice(0, 1)), exchange(random_field, slice(1, channels))]
    row_pads = jnp.repeat(band_pads, BAND)
    span_here = lax.dynamic_slice_in_dim(span_widths, first_row // BAND, rows_here // BAND, 0)
    tables = span_tables(span_here)
    take, give, local = edge_tables(half_widths, row_pads, first_row, rows_here)
    lund = lund_columns(stresses, mean_flow)
    downward = [(i, i + 1) for i in range(wall_count - 1)]
    upward = [(i + 1, i) for i in range(wall_count - 1)]

    def run(size, field, halos, tables, take, give, local, lund):
        held = None
        arrived = []
        for channel in range(channels):
            low, high = halos[min(channel, 1)]
            for half in range(2):
                part = tuple(table[half, :size, :] for table in give)
                *held, send = front(
                    field, low, high, tables, part, held, channel, max(channel - 1, 0), half
                )
                arrived.append(lax.ppermute(send, "wall", upward if half == 0 else downward))
        out = local_filter(held, local, lund)
        for channel in range(channels):
            for half in range(2):
                recv = arrived[2 * channel + 1 - half]
                part = tuple(table[half, :, :size] for table in take)
                out = correct(out, recv, part, lund, channel, half)
        return out

    operands = (random_field, halos, tables, take, give, local, lund)
    if len(SIZES) == 1:
        return run(SIZES[0], *operands)
    needed = rows_needed(half_widths, row_pads, rows_here)
    which = sum((needed > size).astype(jnp.int32) for size in SIZES[:-1])
    return lax.switch(which, [functools.partial(run, size) for size in SIZES], *operands)


def solution(mesh):
    return jax.shard_map(
        shards,
        mesh=mesh,
        in_specs=(P(None, "wall", "span"), P(), P(), P(), P(None, "wall"), P("wall")),
        out_specs=P(None, "wall", "span"),
        check_vma=False,
    )
```

```python
import functools

import jax
import jax.numpy as jnp
from jax import lax
from jax.experimental import pallas as pl
from jax.experimental.pallas import tpu as pltpu
from jax.sharding import PartitionSpec as P

MAXW = 256
SPMAX = 64
BAND = 64
REACH = 2 * SPMAX
TILE = 4 * SPMAX
SIZES = (128, 144, 160, 176, 256)


def split(values):
    high = values.astype(jnp.bfloat16)
    return high, (values - high.astype(jnp.float32)).astype(jnp.bfloat16)


def dot(left, right):
    return lax.dot_general(left, right, (((1,), (0,)), ((), ())), preferred_element_type=jnp.float32)


def dot3(left_high, left_low, right_high, right_low):
    return dot(left_high, right_high) + (dot(left_high, right_low) + dot(left_low, right_high))


def iota(shape, axis):
    return lax.broadcasted_iota(jnp.int32, shape, axis).astype(jnp.float32)


def wall_coeff(distance, rate, pad, inverse):
    return jnp.where(distance <= pad, jnp.exp(distance * distance * rate) * inverse, 0.0)


def rate_of(width):
    return (-0.5 * jnp.pi) / (width * width)


def inverse_norm(width, pad):
    steps = iota((1, MAXW + 128), 1)
    profile = wall_coeff(steps, rate_of(width), pad, 1.0)
    return 1.0 / jnp.sqrt(2.0 * jnp.sum(profile * profile, axis=1, keepdims=True) - 1.0)


def cover(width, pad, depth):
    need = jnp.floor(jnp.minimum(pad, width * 8.25)) - depth
    counts = iota((1, MAXW + 128), 1)
    total = jnp.sum(jnp.where(need > counts, 1.0, 0.0), axis=0, keepdims=True) + counts
    key = jnp.min(jnp.where(counts <= MAXW, total, 4096.0) * 512.0 + counts, axis=1, keepdims=True)
    cost = jnp.floor(key * (1.0 / 512.0))
    best = key - cost * 512.0
    return need, best, cost


def slots(need, best):
    part = jnp.where(need > best, 1.0, 0.0)
    earlier = jnp.where(iota((MAXW, MAXW), 1) < iota((MAXW, MAXW), 0), 1.0, 0.0).astype(jnp.bfloat16)
    before = dot(earlier, jnp.broadcast_to(part, (MAXW, 128)).astype(jnp.bfloat16))[:, :1]
    return jnp.where(part > 0.0, best + before, -1.0)


def early_kernel(segments, span_ref, rows_ref, gh_ref, gl_ref, wh_ref, wl_ref, needed_ref, square_ref):
    band = pl.program_id(0)

    @pl.when(band == 0)
    def _():
        shift = iota((2 * TILE, TILE), 0) - REACH - iota((2 * TILE, TILE), 1)
        square_ref[...] = shift * shift
        columns = jnp.transpose(rows_ref[...])
        column = lambda k: columns[:, k : k + 1]
        index = iota((MAXW, 1), 0)
        lane = iota((1, MAXW), 1)

        for half, segment in ((0, 0), (1, 3)):
            width, pad = column(segment), column(4 + segment)
            depth = MAXW - 1.0 - index if half == 0 else index
            away = lane + 1.0 if half == 0 else MAXW - lane
            need, best, _ = cover(width, pad, depth)
            place = slots(need, best)
            chosen = jnp.where(place == lane, 1.0, 0.0).astype(jnp.bfloat16)
            high, low = split(wall_coeff(depth + away, rate_of(width), pad, inverse_norm(width, pad)))
            pick = lambda values: lax.dot_general(
                chosen, values, (((0,), (0,)), ((), ())), preferred_element_type=jnp.float32
            )
            plain = jnp.where((away == index + 1.0) & (index < best), 1.0, 0.0)
            wh_ref[half] = (pick(high) + plain).astype(jnp.bfloat16)
            wl_ref[half] = pick(low).astype(jnp.bfloat16)

        most = jnp.zeros((1, 1), jnp.float32)
        for segment in range(1, segments - 1):
            depth = MAXW - 1.0 - index if segment % 2 else index
            cost = cover(column(8 + segment), column(8 + segments + segment), depth)[2]
            most = jnp.maximum(most, cost)
        needed_ref[0, 0] = jnp.max(most).astype(jnp.int32)

    spread = jnp.full((1, 1), span_ref[band], jnp.int32).astype(jnp.float32)
    rate = rate_of(spread)
    steps = iota((1, 4 * REACH), 1) - 2 * REACH
    profile = jnp.where(jnp.abs(steps) <= 2.0 * spread, jnp.exp(steps * steps * rate), 0.0)
    inverse = 1.0 / jnp.sqrt(jnp.sum(profile * profile, axis=1, keepdims=True))
    square = square_ref[...]
    coeffs = jnp.where(square <= 4.0 * spread * spread, jnp.exp(square * rate) * inverse, 0.0)
    gh_ref[0], gl_ref[0] = split(coeffs)


def early_tables(span_here, rows, segments):
    bands = span_here.shape[0]
    toeplitz = jax.ShapeDtypeStruct((bands, 2 * TILE, TILE), jnp.bfloat16)
    give = jax.ShapeDtypeStruct((2, MAXW, MAXW), jnp.bfloat16)
    block = pl.BlockSpec((1, 2 * TILE, TILE), lambda b, s: (b, 0, 0))
    whole = pl.BlockSpec((2, MAXW, MAXW), lambda b, s: (0, 0, 0))
    gh, gl, wh, wl, needed = pl.pallas_call(
        functools.partial(early_kernel, segments),
        grid_spec=pltpu.PrefetchScalarGridSpec(
            num_scalar_prefetch=1,
            grid=(bands,),
            in_specs=[pl.BlockSpec(rows.shape, lambda b, s: (0, 0))],
            out_specs=[block, block, whole, whole, pl.BlockSpec(memory_space=pltpu.SMEM)],
            scratch_shapes=[pltpu.VMEM((2 * TILE, TILE), jnp.float32)],
        ),
        out_shape=[toeplitz, toeplitz, give, give, jax.ShapeDtypeStruct((1, 1), jnp.int32)],
        name="early",
    )(span_here, rows)
    return (gh, gl), (wh, wl), needed[0, 0]


def late_kernel(wall_count, where_ref, rows_ref, stress_ref, ah_ref, al_ref, hh_ref, hl_ref, lund_ref):
    columns = jnp.transpose(rows_ref[...])
    column = lambda k: columns[:, k : k + 1]
    index = iota((MAXW, 1), 0)
    lane = iota((1, MAXW), 1)
    for half, segment in ((0, 1), (1, 2)):
        width, pad = column(segment), column(4 + segment)
        rate, inverse = rate_of(width), inverse_norm(width, pad)
        depth = index if half == 0 else MAXW - 1.0 - index
        need, best, _ = cover(width, pad, depth)
        place = slots(need, best)
        plain = wall_coeff(depth + lane + 1.0, rate, pad, inverse)
        plain = jnp.where((place < 0.0) & (lane < best), plain, 0.0)
        take = jnp.where(place == lane, 1.0, plain)
        outer = 0 if half == 0 else wall_count - 1
        take = jnp.where(where_ref[0] == outer, 0.0, take)
        ah_ref[half], al_ref[half] = split(take)
        apart = jnp.abs(iota((1, 2 * MAXW), 1) - (index + half * MAXW))
        rows = slice(half * MAXW, (half + 1) * MAXW)
        hh_ref[rows, :], hl_ref[rows, :] = split(wall_coeff(apart, rate, pad, inverse))

    uu, vv, ww, uv, uw, vw = (stress_ref[k : k + 1, :] for k in range(6))
    lund_aa = jnp.sqrt(uu)
    lund_ba = uv / lund_aa
    lund_bb = jnp.sqrt(vv - lund_ba * lund_ba)
    lund_ca = uw / lund_aa
    lund_cb = (vw - lund_ba * lund_ca) / lund_bb
    lund_cc = jnp.sqrt(ww - lund_ca * lund_ca - lund_cb * lund_cb)
    mean = stress_ref[6:7, :]
    lines = [lund_aa, lund_ba, lund_bb, lund_ca, lund_cb, lund_cc, mean, mean]
    lines.append(jnp.zeros((120, stress_ref.shape[1]), jnp.float32))
    lund_ref[...] = jnp.transpose(jnp.concatenate(lines, axis=0))


def late_tables(where, rows, stress_rows, wall_count):
    rows_here = stress_rows.shape[1]
    take = jax.ShapeDtypeStruct((2, MAXW, MAXW), jnp.bfloat16)
    local = jax.ShapeDtypeStruct((rows_here, rows_here), jnp.bfloat16)
    vmem = pl.BlockSpec(memory_space=pltpu.VMEM)
    ah, al, hh, hl, lund = pl.pallas_call(
        functools.partial(late_kernel, wall_count),
        in_specs=[pl.BlockSpec(memory_space=pltpu.SMEM), vmem, vmem],
        out_specs=[vmem] * 5,
        out_shape=[take, take, local, local, jax.ShapeDtypeStruct((rows_here, 128), jnp.float32)],
        name="late",
    )(where, rows, stress_rows)
    return (ah, al), (hh, hl), lund


def front_kernel(tiles, bands, x_ref, low_ref, high_ref, gh_ref, gl_ref, wh_ref, wl_ref, *rest):
    sh_ref, sl_ref, send_ref, keep_high, keep_low = rest[-5:]
    band = pl.program_id(0)
    wide = jnp.concatenate([low_ref[0], x_ref[0], high_ref[0]], axis=1)
    wide_high, wide_low = split(wide)
    x_high = jnp.concatenate([wide_high[:, t * TILE : (t + 2) * TILE] for t in range(tiles)], axis=0)
    x_low = jnp.concatenate([wide_low[:, t * TILE : (t + 2) * TILE] for t in range(tiles)], axis=0)
    high, low = split(dot3(x_high, x_low, gh_ref[0], gl_ref[0]))
    start = pl.multiple_of(band * BAND, BAND)
    for t in range(tiles):
        cols = slice(t * TILE, (t + 1) * TILE)
        rows = slice(t * BAND, (t + 1) * BAND)
        sh_ref[0, :, cols] = high[rows]
        sl_ref[0, :, cols] = low[rows]
        keep_high[pl.ds(start, BAND), cols] = high[rows]
        keep_low[pl.ds(start, BAND), cols] = low[rows]

    @pl.when(band == bands - 1)
    def _():
        step = 2 * TILE
        for t in range(tiles // 2):
            cols = slice(t * step, (t + 1) * step)
            send_ref[:, cols] = dot3(wh_ref[0], wl_ref[0], keep_high[:, cols], keep_low[:, cols])


def front(size, field, low, high, tables, give, held, channel, halo_channel, half):
    channels, rows, cols = field.shape
    bands = MAXW // BAND
    tiles = cols // TILE
    first = half * (rows // BAND - bands)
    halo = pl.BlockSpec((1, BAND, REACH), lambda b: (halo_channel, first + b, 0))
    toeplitz = pl.BlockSpec((1, 2 * TILE, TILE), lambda b: (first + b, 0, 0))
    send = pl.BlockSpec((1, size, MAXW), lambda b: (half, 0, 0))
    block = pl.BlockSpec((1, BAND, cols), lambda b: (channel, first + b, 0))
    in_specs = [block, halo, halo, toeplitz, toeplitz, send, send]
    operands = [field, low, high, *tables, *give]
    aliases = {}
    if held is not None:
        in_specs += [pl.BlockSpec(memory_space=pl.ANY)] * 2
        aliases = {len(operands): 0, len(operands) + 1: 1}
        operands += list(held)
    kept = jax.ShapeDtypeStruct((channels, rows, cols), jnp.bfloat16)
    return pl.pallas_call(
        functools.partial(front_kernel, tiles, bands),
        grid=(bands,),
        in_specs=in_specs,
        out_specs=[block, block, pl.BlockSpec((size, cols), lambda b: (0, 0))],
        out_shape=[kept, kept, jax.ShapeDtypeStruct((size, cols), jnp.float32)],
        scratch_shapes=[pltpu.VMEM((MAXW, cols), jnp.bfloat16)] * 2,
        input_output_aliases=aliases,
        cost_estimate=pl.CostEstimate(
            flops=6 * MAXW * cols * 2 * TILE + 6 * size * MAXW * cols,
            bytes_accessed=MAXW * cols * 8 + size * cols * 4,
            transcendentals=0,
        ),
        name="front",
    )(*operands)


def across(ah_ref, al_ref, half, recv):
    size = recv.shape[0]
    high, low = split(recv)
    return dot3(ah_ref[half, :, :size], al_ref[half, :, :size], high, low)


def main_kernel(sh_ref, sl_ref, top0, low0, top1, low1, ah_ref, al_ref, hh_ref, hl_ref, lund_ref, out_ref):
    rows = sh_ref.shape[1]
    column = lambda k: lund_ref[:, k : k + 1]

    def psi(channel, top=None, bottom=None):
        value = dot3(hh_ref[...], hl_ref[...], sh_ref[channel], sl_ref[channel])
        if top is None:
            return value
        above = across(ah_ref, al_ref, 0, top[...])
        below = across(ah_ref, al_ref, 1, bottom[...])
        return jnp.concatenate([value[:MAXW] + above, value[rows - MAXW :] + below], axis=0)

    first = psi(0, top0, low0)
    out_ref[0] = column(6) + column(0) * first
    second = psi(1, top1, low1)
    out_ref[1] = column(1) * first + column(2) * second
    out_ref[2] = column(3) * first + column(4) * second + column(5) * psi(2)


def main_filter(held, arrived, take, local, lund):
    channels, rows, cols = held[0].shape
    size = arrived[0].shape[0]
    step = TILE
    block = pl.BlockSpec((channels, rows, step), lambda t: (0, 0, t))
    whole = lambda array: pl.BlockSpec(array.shape, lambda t: (0,) * array.ndim)
    return pl.pallas_call(
        main_kernel,
        grid=(cols // step,),
        in_specs=[block, block]
        + [pl.BlockSpec((size, step), lambda t: (0, t))] * 4
        + [whole(array) for array in (*take, *local, lund)],
        out_specs=block,
        out_shape=jax.ShapeDtypeStruct((channels, rows, cols), jnp.float32),
        cost_estimate=pl.CostEstimate(
            flops=6 * channels * rows * rows * cols, bytes_accessed=channels * rows * cols * 8, transcendentals=0
        ),
        name="main",
    )(*held, *arrived, *take, *local, lund)


def tail_kernel(top, bottom, ah_ref, al_ref, lund_ref, out_in_ref, out_ref):
    rows = out_ref.shape[1]
    for half, recv in ((0, top), (1, bottom)):
        part = slice(0, MAXW) if half == 0 else slice(rows - MAXW, rows)
        out_ref[0, part, :] = out_in_ref[0, part, :] + lund_ref[part, 5:6] * across(ah_ref, al_ref, half, recv[...])


def tail_filter(out, arrived, take, lund):
    channels, rows, cols = out.shape
    size = arrived[0].shape[0]
    step = TILE
    block = pl.BlockSpec((1, rows, step), lambda t: (channels - 1, 0, t))
    whole = lambda array: pl.BlockSpec(array.shape, lambda t: (0,) * array.ndim)
    return pl.pallas_call(
        tail_kernel,
        grid=(cols // step,),
        in_specs=[pl.BlockSpec((size, step), lambda t: (0, t))] * 2
        + [whole(array) for array in (*take, lund)]
        + [block],
        out_specs=block,
        out_shape=jax.ShapeDtypeStruct(out.shape, out.dtype),
        input_output_aliases={5: 0},
        cost_estimate=pl.CostEstimate(
            flops=6 * rows * size * cols, bytes_accessed=rows * cols * 8 + size * cols * 8, transcendentals=0
        ),
        name="tail",
    )(*arrived, *take, lund, out)


def ring(axis):
    count = lax.axis_size(axis)
    forward = [(i, (i + 1) % count) for i in range(count)]
    return forward, [(target, source) for source, target in forward]


def exchange(edges):
    forward, backward = ring("span")
    return lax.ppermute(edges[1], "span", forward), lax.ppermute(edges[0], "span", backward)


def shards(random_field, half_widths, band_pads, span_widths, stresses, mean_flow):
    channels, rows_here, _ = random_field.shape
    wall_count = lax.axis_size("wall")
    where = lax.axis_index("wall")
    edges = [
        (random_field[part, :, :REACH], random_field[part, :, -REACH:])
        for part in (slice(0, 1), slice(1, channels))
    ]
    first_halo = exchange(edges[0])

    segments = half_widths.shape[0] // MAXW
    span_here = lax.dynamic_slice_in_dim(
        span_widths, where * (rows_here // BAND), rows_here // BAND, 0
    )
    plane = jnp.stack([half_widths, jnp.repeat(band_pads, BAND)], axis=0).astype(jnp.float32)
    plane = plane.reshape(2, segments, MAXW)
    padded = jnp.pad(plane, ((0, 0), (1, 1), (0, 0)), constant_values=1.0)
    window = lax.dynamic_slice_in_dim(padded, where * (rows_here // MAXW), rows_here // MAXW + 2, 1)
    rows = jnp.concatenate([window.reshape(-1, MAXW), plane.reshape(-1, MAXW)], axis=0)
    rows = jnp.pad(rows, ((0, 128 - rows.shape[0]), (0, 0)), constant_values=1.0)
    stress_rows = jnp.pad(jnp.concatenate([stresses, mean_flow[None]], axis=0), ((0, 1), (0, 0)))

    tables, give, needed = early_tables(span_here, rows, segments)
    downward, upward = ring("wall")

    def run(size, field, halo, edges, tables, give, where, rows, stress_rows):
        halos = [halo, exchange(edges)]
        held = None
        arrived = []
        for channel in range(channels):
            low, high = halos[min(channel, 1)]
            for half in range(2):
                *held, send = front(
                    size, field, low, high, tables, give, held, channel, max(channel - 1, 0), half
                )
                arrived.append(lax.ppermute(send, "wall", upward if half == 0 else downward))
        take, local, lund = late_tables(where, rows, stress_rows, wall_count)
        tops, bottoms = arrived[1::2], arrived[0::2]
        out = main_filter(held, (tops[0], bottoms[0], tops[1], bottoms[1]), take, local, lund)
        return tail_filter(out, (tops[2], bottoms[2]), take, lund)

    operands = (
        random_field, first_halo, edges[1], tables, give, where.reshape(1), rows, stress_rows
    )
    if len(SIZES) == 1:
        return run(SIZES[0], *operands)
    which = sum((needed > size).astype(jnp.int32) for size in SIZES[:-1])
    return lax.switch(which, [functools.partial(run, size) for size in SIZES], *operands)


def solution(mesh):
    return jax.shard_map(
        shards,
        mesh=mesh,
        in_specs=(P(None, "wall", "span"), P(), P(), P(), P(None, "wall"), P("wall")),
        out_specs=P(None, "wall", "span"),
        check_vma=False,
    )
```

```python
import functools

import jax
import jax.numpy as jnp
from jax import lax
from jax.experimental import pallas as pl
from jax.experimental.pallas import tpu as pltpu
from jax.sharding import PartitionSpec as P

MAXW = 256
SPMAX = 64
BAND = 64
REACH = 2 * SPMAX
TILE = 4 * SPMAX
SIZES = (152, 184, 256)


def split(values):
    high = values.astype(jnp.bfloat16)
    return high, (values - high.astype(jnp.float32)).astype(jnp.bfloat16)


def dot(left, right):
    return lax.dot_general(left, right, (((1,), (0,)), ((), ())), preferred_element_type=jnp.float32)


def dot3(left_high, left_low, right_high, right_low):
    return dot(left_high, right_high) + (dot(left_high, right_low) + dot(left_low, right_high))


def whole(array):
    return pl.BlockSpec(array.shape, lambda *_: (0,) * len(array.shape))


def iota(shape, axis):
    return lax.broadcasted_iota(jnp.int32, shape, axis).astype(jnp.float32)


def wall_coeff(distance, rate, pad, inverse):
    return jnp.where(distance <= pad, jnp.exp(distance * distance * rate) * inverse, 0.0)


def rate_of(width):
    return (-0.5 * jnp.pi) / (width * width)


def inverse_norm(width, pad):
    steps = iota((1, MAXW + 128), 1)
    profile = wall_coeff(steps, rate_of(width), pad, 1.0)
    return 1.0 / jnp.sqrt(2.0 * jnp.sum(profile * profile, axis=1, keepdims=True) - 1.0)


def cover(width, pad, depth):
    need = jnp.floor(jnp.minimum(pad, width * 8.25)) - depth
    counts = iota((1, MAXW + 128), 1)
    total = jnp.sum(jnp.where(need > counts, 1.0, 0.0), axis=0, keepdims=True) + counts
    key = jnp.min(jnp.where(counts <= MAXW, total, 4096.0) * 512.0 + counts, axis=1, keepdims=True)
    cost = jnp.floor(key * (1.0 / 512.0))
    best = key - cost * 512.0
    return need, best, cost


def slots(need, best):
    part = jnp.where(need > best, 1.0, 0.0)
    earlier = jnp.where(iota((MAXW, MAXW), 1) < iota((MAXW, MAXW), 0), 1.0, 0.0).astype(jnp.bfloat16)
    before = dot(earlier, jnp.broadcast_to(part, (MAXW, 128)).astype(jnp.bfloat16))[:, :1]
    return jnp.where(part > 0.0, best + before, -1.0)


def early_kernel(
    segments, where_ref, pads_ref, span_ref, widths_ref, gh_ref, gl_ref, wh_ref, wl_ref, rows_ref, needed_ref,
    square_ref, plane_ref,
):
    band = pl.program_id(0)
    where = where_ref[0]
    per = MAXW // BAND

    @pl.when(band == 0)
    def _():
        shift = iota((3 * REACH, REACH), 0) - REACH - iota((3 * REACH, REACH), 1)
        square_ref[...] = shift * shift
        plane_ref[...] = jnp.ones(plane_ref.shape, jnp.float32)
        plane_ref[0, 1 : segments + 1, :] = widths_ref[...].astype(jnp.float32)
        lanes = lax.broadcasted_iota(jnp.int32, (1, MAXW), 1)
        for segment in range(segments):
            line = jnp.full((1, MAXW), pads_ref[segment * per], jnp.int32)
            for k in range(1, per):
                line = jnp.where(lanes >= k * BAND, pads_ref[segment * per + k], line)
            plane_ref[1, segment + 1 : segment + 2, :] = line.astype(jnp.float32)
        rows_ref[...] = jnp.ones(rows_ref.shape, jnp.float32)
        for k in range(2):
            for j in range(4):
                rows_ref[4 * k + j : 4 * k + j + 1, :] = plane_ref[k, pl.ds(2 * where + j, 1), :]
            rows_ref[8 + k * segments : 8 + (k + 1) * segments, :] = plane_ref[k, 1 : segments + 1, :]
        columns = jnp.transpose(rows_ref[...])
        column = lambda k: columns[:, k : k + 1]
        index = iota((MAXW, 1), 0)
        lane = iota((1, MAXW), 1)

        for half, segment in ((0, 0), (1, 3)):
            width, pad = column(segment), column(4 + segment)
            depth = MAXW - 1.0 - index if half == 0 else index
            away = lane + 1.0 if half == 0 else MAXW - lane
            need, best, _ = cover(width, pad, depth)
            place = slots(need, best)
            chosen = jnp.where(place == lane, 1.0, 0.0).astype(jnp.bfloat16)
            high, low = split(wall_coeff(depth + away, rate_of(width), pad, inverse_norm(width, pad)))
            pick = lambda values: lax.dot_general(
                chosen, values, (((0,), (0,)), ((), ())), preferred_element_type=jnp.float32
            )
            plain = jnp.where((away == index + 1.0) & (index < best), 1.0, 0.0)
            wh_ref[half] = (pick(high) + plain).astype(jnp.bfloat16)
            wl_ref[half] = pick(low).astype(jnp.bfloat16)

        most = jnp.zeros((1, 1), jnp.float32)
        for segment in range(1, segments - 1):
            depth = MAXW - 1.0 - index if segment % 2 else index
            cost = cover(column(8 + segment), column(8 + segments + segment), depth)[2]
            most = jnp.maximum(most, cost)
        needed_ref[0, 0] = jnp.max(most).astype(jnp.int32)

    spread = jnp.full((1, 1), span_ref[where * pl.num_programs(0) + band], jnp.int32).astype(jnp.float32)
    rate = rate_of(spread)
    steps = iota((1, 4 * REACH), 1) - 2 * REACH
    profile = jnp.where(jnp.abs(steps) <= 2.0 * spread, jnp.exp(steps * steps * rate), 0.0)
    inverse = 1.0 / jnp.sqrt(jnp.sum(profile * profile, axis=1, keepdims=True))
    square = square_ref[...]
    coeffs = jnp.where(square <= 4.0 * spread * spread, jnp.exp(square * rate) * inverse, 0.0)
    gh_ref[0], gl_ref[0] = split(coeffs)


def early_tables(where, band_pads, span_widths, half_widths, bands):
    segments = half_widths.shape[0]
    toeplitz = jax.ShapeDtypeStruct((bands, 3 * REACH, REACH), jnp.bfloat16)
    give = jax.ShapeDtypeStruct((2, MAXW, MAXW), jnp.bfloat16)
    rows = jax.ShapeDtypeStruct((128, MAXW), jnp.float32)
    block = pl.BlockSpec((1, 3 * REACH, REACH), lambda b, *s: (b, 0, 0))
    whole = pl.BlockSpec((2, MAXW, MAXW), lambda b, *s: (0, 0, 0))
    gh, gl, wh, wl, rows, needed = pl.pallas_call(
        functools.partial(early_kernel, segments),
        grid_spec=pltpu.PrefetchScalarGridSpec(
            num_scalar_prefetch=3,
            grid=(bands,),
            in_specs=[pl.BlockSpec(half_widths.shape, lambda b, *s: (0, 0))],
            out_specs=[
                block, block, whole, whole,
                pl.BlockSpec(rows.shape, lambda b, *s: (0, 0)),
                pl.BlockSpec(memory_space=pltpu.SMEM),
            ],
            scratch_shapes=[
                pltpu.VMEM((3 * REACH, REACH), jnp.float32),
                pltpu.VMEM((2, segments + 8, MAXW), jnp.float32),
            ],
        ),
        out_shape=[toeplitz, toeplitz, give, give, rows, jax.ShapeDtypeStruct((1, 1), jnp.int32)],
        name="early",
    )(where, band_pads, span_widths, half_widths)
    return (gh, gl), (wh, wl), rows, needed[0, 0]


def late_kernel(where_ref, rows_ref, stress_ref, ah_ref, al_ref, hh_ref, hl_ref, lund_ref):
    half = pl.program_id(0)
    last = pl.num_programs(0) - 1
    stand = lambda k: jnp.transpose(jnp.broadcast_to(rows_ref[pl.ds(k, 1), :], (128, MAXW)))[:, :1]
    width, pad = stand(1 + half), stand(5 + half)
    index = iota((MAXW, 1), 0)
    lane = iota((1, MAXW), 1)
    rate, inverse = rate_of(width), inverse_norm(width, pad)
    depth = jnp.where(half == 0, index, MAXW - 1.0 - index)
    need, best, _ = cover(width, pad, depth)
    place = slots(need, best)
    plain = wall_coeff(depth + lane + 1.0, rate, pad, inverse)
    plain = jnp.where((place < 0.0) & (lane < best), plain, 0.0)
    take = jnp.where(place == lane, 1.0, plain)
    outer = jnp.where(half == 0, where_ref[0] == 0, where_ref[0] == where_ref[1] - 1)
    take = jnp.where(outer, 0.0, take)
    ah_ref[0], al_ref[0] = split(take)
    apart = jnp.abs(iota((1, 2 * MAXW), 1) - (index + (half * MAXW).astype(jnp.float32)))
    hh_ref[...], hl_ref[...] = split(wall_coeff(apart, rate, pad, inverse))

    @pl.when(half == last)
    def _():
        uu, vv, ww, uv, uw, vw = (stress_ref[k : k + 1, :] for k in range(6))
        lund_aa = jnp.sqrt(uu)
        lund_ba = uv / lund_aa
        lund_bb = jnp.sqrt(vv - lund_ba * lund_ba)
        lund_ca = uw / lund_aa
        lund_cb = (vw - lund_ba * lund_ca) / lund_bb
        lund_cc = jnp.sqrt(ww - lund_ca * lund_ca - lund_cb * lund_cb)
        mean = stress_ref[6:7, :]
        lines = [lund_aa, lund_ba, lund_bb, lund_ca, lund_cb, lund_cc, mean, mean]
        lines.append(jnp.zeros((120, stress_ref.shape[1]), jnp.float32))
        lund_ref[...] = jnp.transpose(jnp.concatenate(lines, axis=0))


def late_tables(where, rows, stress_rows):
    rows_here = stress_rows.shape[1]
    take = jax.ShapeDtypeStruct((2, MAXW, MAXW), jnp.bfloat16)
    local = jax.ShapeDtypeStruct((rows_here, rows_here), jnp.bfloat16)
    take_block = pl.BlockSpec((1, MAXW, MAXW), lambda h: (h, 0, 0))
    local_block = pl.BlockSpec((MAXW, rows_here), lambda h: (h, 0))
    ah, al, hh, hl, lund = pl.pallas_call(
        late_kernel,
        grid=(2,),
        in_specs=[pl.BlockSpec(memory_space=pltpu.SMEM), whole(rows), whole(stress_rows)],
        out_specs=[take_block, take_block, local_block, local_block, pl.BlockSpec((rows_here, 128), lambda h: (0, 0))],
        out_shape=[take, take, local, local, jax.ShapeDtypeStruct((rows_here, 128), jnp.float32)],
        name="late",
    )(where, rows, stress_rows)
    return (ah, al), (hh, hl), lund


def widened(block):
    zero = jnp.zeros((REACH, REACH), block.dtype)
    left = jnp.concatenate([block, zero], axis=0)
    return jnp.concatenate([left, jnp.concatenate([zero, block], axis=0)], axis=1)


def front_kernel(tile_range, pieces, x_ref, low_ref, high_ref, gh_ref, gl_ref, wh_ref, wl_ref, *rest):
    keep_high, keep_low = rest[-2:]
    sh_ref, sl_ref, *sends = rest[-4 - 2 * len(pieces) : -2]
    band = pl.program_id(0)
    per = MAXW // BAND
    first, last = tile_range
    wide = jnp.concatenate([low_ref[0], x_ref[0], high_ref[0]], axis=1)[:, first * TILE : (last + 1) * TILE]
    wide_high, wide_low = split(wide)
    count = last - first
    x_high = jnp.concatenate([wide_high[:, t * TILE : (t + 2) * TILE] for t in range(count)], axis=0)
    x_low = jnp.concatenate([wide_low[:, t * TILE : (t + 2) * TILE] for t in range(count)], axis=0)
    high, low = split(dot3(x_high, x_low, widened(gh_ref[0]), widened(gl_ref[0])))
    start = pl.multiple_of((band % per) * BAND, BAND)
    for t in range(count):
        cols = slice(t * TILE, (t + 1) * TILE)
        rows = slice(t * BAND, (t + 1) * BAND)
        sh_ref[0, :, cols] = high[rows]
        sl_ref[0, :, cols] = low[rows]
        keep_high[pl.ds(start, BAND), cols] = high[rows]
        keep_low[pl.ds(start, BAND), cols] = low[rows]

    for half in range(2):

        @pl.when(band == (per - 1 if half == 0 else pl.num_programs(0) - 1))
        def _(half=half):
            step = TILE
            for (left, right, top, end), send_ref in zip(pieces, sends[half::2]):

                def body(t, carry, left=left, top=top, end=end, send_ref=send_ref):
                    here = pl.ds(pl.multiple_of(t * step, step), step)
                    cols = pl.ds(pl.multiple_of(t * step + left, step), step)
                    send_ref[:, here] = dot3(
                        wh_ref[0, top:end, :], wl_ref[0, top:end, :], keep_high[:, cols], keep_low[:, cols]
                    )
                    return carry

                lax.fori_loop(0, (right - left) // step, body, 0)


def front(spans, field, low, high, tables, give, held, channel, cuts):
    channels, rows, cols = field.shape
    bands = rows // BAND
    tiles = cols // TILE
    width = cols // cuts
    size = spans[-1][1]
    pieces = [(k * width, (k + 1) * width, *span) for k in range(cuts) for span in spans]
    halo = pl.BlockSpec((1, BAND, REACH), lambda b: (max(channel - 1, 0), b, 0))
    toeplitz = pl.BlockSpec((1, 3 * REACH, REACH), lambda b: (b, 0, 0))
    half = pl.BlockSpec((1, size, MAXW), lambda b: (b * 2 // bands, 0, 0))
    line = pl.BlockSpec((1, BAND, cols), lambda b: (channel, b, 0))
    block = line
    in_specs = [line, halo, halo, toeplitz, toeplitz, half, half]
    operands = [field, low, high, *tables, *give]
    aliases = {}
    if held is not None:
        in_specs += [pl.BlockSpec(memory_space=pl.ANY)] * 2
        aliases = {len(operands): 0, len(operands) + 1: 1}
        operands += list(held)
    kept = jax.ShapeDtypeStruct((channels, rows, cols), jnp.bfloat16)
    sends = [jax.ShapeDtypeStruct((p[3] - p[2], width), jnp.float32) for p in pieces for _ in range(2)]
    results = pl.pallas_call(
        functools.partial(front_kernel, (0, tiles), pieces),
        grid=(bands,),
        in_specs=in_specs,
        out_specs=[block, block] + [whole(send) for send in sends],
        out_shape=[kept, kept] + sends,
        scratch_shapes=[pltpu.VMEM((MAXW, cols), jnp.bfloat16)] * 2,
        input_output_aliases=aliases,
        cost_estimate=pl.CostEstimate(
            flops=6 * rows * cols * 2 * TILE + 12 * size * MAXW * cols,
            bytes_accessed=rows * cols * 8 + size * cols * 8,
            transcendentals=0,
        ),
        name="front",
    )(*operands)
    return results[:2], [tuple(results[2 + 2 * k : 4 + 2 * k]) for k in range(len(pieces))]


def across(ah_ref, al_ref, half, recv):
    size = recv.shape[0]
    high, low = split(recv)
    return dot3(ah_ref[half, :, :size], al_ref[half, :, :size], high, low)


def main_kernel(counts, sh_ref, sl_ref, *rest):
    arrived = rest[: 2 * sum(counts)]
    ah_ref, al_ref, hh_ref, hl_ref, lund_ref, out_ref = rest[2 * sum(counts) :]

    def body(channel, carry):
        out_ref[channel] = dot3(hh_ref[...], hl_ref[...], sh_ref[channel], sl_ref[channel])
        return carry

    lax.fori_loop(0, sh_ref.shape[0], body, 0)

    def psi(channel):
        start = 2 * sum(counts[:channel])
        sums = []
        for half in range(2):
            parts = [ref[...] for ref in arrived[start + half : start + 2 * counts[channel] : 2]]
            sums.append(across(ah_ref, al_ref, half, jnp.concatenate(parts, axis=0)))
        return out_ref[channel] + jnp.concatenate(sums, axis=0)

    column = lambda k: lund_ref[:, k : k + 1]
    first, second = psi(0), psi(1)
    out_ref[0] = column(6) + column(0) * first
    out_ref[1] = column(1) * first + column(2) * second
    out_ref[2] = column(3) * first + column(4) * second + column(5) * out_ref[2]


ROOM = pltpu.CompilerParams(vmem_limit_bytes=56 * 1024 * 1024)


def main_filter(held, arrived, take, local, lund):
    channels, rows, cols = held[0].shape
    counts = tuple(len(pieces) for pieces in arrived)
    recv = [array for pieces in arrived for pair in pieces for array in pair]
    step = TILE
    block = pl.BlockSpec((channels, rows, step), lambda t: (0, 0, t))
    return pl.pallas_call(
        functools.partial(main_kernel, counts),
        grid=(cols // step,),
        in_specs=[block, block]
        + [pl.BlockSpec((array.shape[0], step), lambda t: (0, t)) for array in recv]
        + [whole(array) for array in (*take, *local, lund)],
        out_specs=block,
        out_shape=jax.ShapeDtypeStruct((channels, rows, cols), jnp.float32),
        compiler_params=ROOM,
        cost_estimate=pl.CostEstimate(
            flops=6 * channels * rows * rows * cols, bytes_accessed=channels * rows * cols * 8, transcendentals=0
        ),
        name="main",
    )(*held, *recv, *take, *local, lund)


def update_kernel(top, bottom, ah_ref, al_ref, lund_ref, out_in_ref, out_ref):
    def body(t, carry):
        cols = pl.ds(pl.multiple_of(t * TILE, TILE), TILE)
        for half, recv in ((0, top), (1, bottom)):
            rows = slice(half * MAXW, (half + 1) * MAXW)
            given = lund_ref[rows, 5:6] * across(ah_ref, al_ref, half, recv[:, cols])
            out_ref[0, rows, cols] = out_in_ref[0, rows, cols] + given
        return carry

    lax.fori_loop(0, out_ref.shape[2] // TILE, body, 0)


def update(out, arrived, take, lund, first):
    channels, rows, _ = out.shape
    size, width = arrived[0].shape
    step = 2 * TILE
    block = pl.BlockSpec((1, rows, step), lambda t: (channels - 1, 0, t + first // step))
    return pl.pallas_call(
        update_kernel,
        grid=(width // step,),
        in_specs=[pl.BlockSpec((size, step), lambda t: (0, t))] * 2
        + [whole(array) for array in (*take, lund)]
        + [block],
        out_specs=block,
        out_shape=jax.ShapeDtypeStruct(out.shape, out.dtype),
        input_output_aliases={5: 0},
        compiler_params=ROOM,
        cost_estimate=pl.CostEstimate(
            flops=6 * rows * size * width, bytes_accessed=rows * width * 8 + size * width * 8, transcendentals=0
        ),
        name="update",
    )(*arrived, *take, lund, out)


def ring(axis):
    count = lax.axis_size(axis)
    forward = [(i, (i + 1) % count) for i in range(count)]
    return forward, [(target, source) for source, target in forward]


def exchange(field):
    forward, backward = ring("span")
    low = lax.ppermute(field[:, :, -REACH:], "span", forward)
    return low, lax.ppermute(field[:, :, :REACH], "span", backward)


def shards(random_field, half_widths, band_pads, span_widths, stresses, mean_flow):
    _, rows_here, cols = random_field.shape
    wall_count = lax.axis_size("wall")
    where = jnp.stack([lax.axis_index("wall"), jnp.int32(wall_count)])
    halo = exchange(random_field[:1])
    tables, give, rows, needed = early_tables(
        where, band_pads, span_widths, half_widths.reshape(-1, MAXW), rows_here // BAND
    )
    rest, needed = lax.optimization_barrier((random_field, needed))
    halos = exchange(rest[1:])
    stress_rows = jnp.pad(jnp.concatenate([stresses, mean_flow[None]], axis=0), ((0, 1), (0, 0)))
    downward, upward = ring("wall")
    spans = list(zip((0,) + SIZES[:-1], SIZES))
    held, ahead = front(spans, random_field, *halo, tables, give, None, 0, 1)

    def across_edges(pieces):
        arrived = []
        for up, down in pieces:
            bottom = lax.ppermute(up, "wall", upward)
            arrived.append((lax.ppermute(down, "wall", downward), bottom))
        return arrived

    def run(number, *operands):
        return steps(number, *operands)

    def steps(number, field, halos, tables, give, where, rows, stress_rows, held, ahead):
        span = [(0, SIZES[number])]
        first = across_edges(ahead[: number + 1])
        held, pieces = front(span, field, *halos, tables, give, held, 1, 1)
        second = across_edges(pieces)
        held, pieces = front(span, field, *halos, tables, give, held, 2, 2)
        third = across_edges(pieces)
        take, local, lund = late_tables(where, rows, stress_rows)
        out = main_filter(held, (first, second), take, local, lund)
        for k, pair in enumerate(third):
            out = update(out, pair, take, lund, k * (cols // len(third)))
        return out

    operands = (random_field, halos, tables, give, where, rows, stress_rows, held, ahead)
    if len(SIZES) == 1:
        return run(0, *operands)
    which = sum((needed > size).astype(jnp.int32) for size in SIZES[:-1])
    return lax.switch(which, [functools.partial(run, k) for k in range(len(SIZES))], *operands)


def solution(mesh):
    return jax.shard_map(
        shards,
        mesh=mesh,
        in_specs=(P(None, "wall", "span"), P(), P(), P(), P(None, "wall"), P("wall")),
        out_specs=P(None, "wall", "span"),
        check_vma=False,
    )
```

```python
import functools

import jax
import jax.numpy as jnp
from jax import lax
from jax.experimental import pallas as pl
from jax.experimental.pallas import tpu as pltpu
from jax.sharding import PartitionSpec as P

MAXW = 256
SPMAX = 64
BAND = 64
REACH = 2 * SPMAX
TILE = 4 * SPMAX
SIZES = (152, 184, 256)


def split(values):
    high = values.astype(jnp.bfloat16)
    return high, (values - high.astype(jnp.float32)).astype(jnp.bfloat16)


def dot(left, right):
    return lax.dot_general(left, right, (((1,), (0,)), ((), ())), preferred_element_type=jnp.float32)


def dot3(left_high, left_low, right_high, right_low):
    return dot(left_high, right_high) + (dot(left_high, right_low) + dot(left_low, right_high))


def whole(array):
    return pl.BlockSpec(array.shape, lambda *_: (0,) * len(array.shape))


def iota(shape, axis):
    return lax.broadcasted_iota(jnp.int32, shape, axis).astype(jnp.float32)


def wall_coeff(distance, rate, pad, inverse):
    return jnp.where(distance <= pad, jnp.exp(distance * distance * rate) * inverse, 0.0)


def rate_of(width):
    return (-0.5 * jnp.pi) / (width * width)


def inverse_norm(width, pad):
    steps = iota((1, MAXW + 128), 1)
    profile = wall_coeff(steps, rate_of(width), pad, 1.0)
    return 1.0 / jnp.sqrt(2.0 * jnp.sum(profile * profile, axis=1, keepdims=True) - 1.0)


def cover(width, pad, depth):
    need = jnp.floor(jnp.minimum(pad, width * 8.25)) - depth
    counts = iota((1, MAXW + 128), 1)
    total = jnp.sum(jnp.where(need > counts, 1.0, 0.0), axis=0, keepdims=True) + counts
    key = jnp.min(jnp.where(counts <= MAXW, total, 4096.0) * 512.0 + counts, axis=1, keepdims=True)
    cost = jnp.floor(key * (1.0 / 512.0))
    best = key - cost * 512.0
    return need, best, cost


def slots(need, best):
    part = jnp.where(need > best, 1.0, 0.0)
    earlier = jnp.where(iota((MAXW, MAXW), 1) < iota((MAXW, MAXW), 0), 1.0, 0.0).astype(jnp.bfloat16)
    before = dot(earlier, jnp.broadcast_to(part, (MAXW, 128)).astype(jnp.bfloat16))[:, :1]
    return jnp.where(part > 0.0, best + before, -1.0)


def early_kernel(
    segments, where_ref, pads_ref, widths_ref, wh_ref, wl_ref, rows_ref, needed_ref, plane_ref
):
    where = where_ref[0]
    per = MAXW // BAND

    plane_ref[...] = jnp.ones(plane_ref.shape, jnp.float32)
    widths = widths_ref[...].astype(jnp.float32)
    split_by = MAXW // widths.shape[1]
    lanes = lax.broadcasted_iota(jnp.int32, (1, MAXW), 1)
    for segment in range(segments):
        parts = [widths[segment * split_by + k : segment * split_by + k + 1] for k in range(split_by)]
        plane_ref[0, segment + 1 : segment + 2, :] = jnp.concatenate(parts, axis=1)
        line = jnp.full((1, MAXW), pads_ref[segment * per], jnp.int32)
        for k in range(1, per):
            line = jnp.where(lanes >= k * BAND, pads_ref[segment * per + k], line)
        plane_ref[1, segment + 1 : segment + 2, :] = line.astype(jnp.float32)
    rows_ref[...] = jnp.ones(rows_ref.shape, jnp.float32)
    for k in range(2):
        for j in range(4):
            rows_ref[4 * k + j : 4 * k + j + 1, :] = plane_ref[k, pl.ds(2 * where + j, 1), :]
        rows_ref[8 + k * segments : 8 + (k + 1) * segments, :] = plane_ref[k, 1 : segments + 1, :]
    columns = jnp.transpose(rows_ref[...])
    column = lambda k: columns[:, k : k + 1]
    index = iota((MAXW, 1), 0)
    lane = iota((1, MAXW), 1)

    for half, segment in ((0, 0), (1, 3)):
        width, pad = column(segment), column(4 + segment)
        depth = MAXW - 1.0 - index if half == 0 else index
        away = lane + 1.0 if half == 0 else MAXW - lane
        need, best, _ = cover(width, pad, depth)
        place = slots(need, best)
        chosen = jnp.where(place == lane, 1.0, 0.0).astype(jnp.bfloat16)
        high, low = split(wall_coeff(depth + away, rate_of(width), pad, inverse_norm(width, pad)))
        pick = lambda values: lax.dot_general(
            chosen, values, (((0,), (0,)), ((), ())), preferred_element_type=jnp.float32
        )
        plain = jnp.where((away == index + 1.0) & (index < best), 1.0, 0.0)
        wh_ref[half] = (pick(high) + plain).astype(jnp.bfloat16)
        wl_ref[half] = pick(low).astype(jnp.bfloat16)

    most = jnp.zeros((1, 1), jnp.float32)
    for segment in range(1, segments - 1):
        depth = MAXW - 1.0 - index if segment % 2 else index
        cost = cover(column(8 + segment), column(8 + segments + segment), depth)[2]
        most = jnp.maximum(most, cost)
    needed_ref[0, 0] = jnp.max(most).astype(jnp.int32)


def early_tables(where, band_pads, half_widths):
    segments = half_widths.shape[0] // MAXW
    half_widths = half_widths.reshape(-1, 128)
    give = jax.ShapeDtypeStruct((2, MAXW, MAXW), jnp.bfloat16)
    rows = jax.ShapeDtypeStruct((128, MAXW), jnp.float32)
    smem = pl.BlockSpec(memory_space=pltpu.SMEM)
    vmem = pl.BlockSpec(memory_space=pltpu.VMEM)
    wh, wl, rows, needed = pl.pallas_call(
        functools.partial(early_kernel, segments),
        in_specs=[smem, smem, vmem],
        out_specs=[vmem, vmem, vmem, smem],
        out_shape=[give, give, rows, jax.ShapeDtypeStruct((1, 1), jnp.int32)],
        scratch_shapes=[pltpu.VMEM((2, segments + 8, MAXW), jnp.float32)],
        name="early",
    )(where, band_pads, half_widths)
    return (wh, wl), rows, needed[0, 0]


def late_kernel(where_ref, rows_ref, stress_ref, ah_ref, al_ref, hh_ref, hl_ref, lund_ref):
    half = pl.program_id(0)
    last = pl.num_programs(0) - 1
    stand = lambda k: jnp.transpose(jnp.broadcast_to(rows_ref[pl.ds(k, 1), :], (128, MAXW)))[:, :1]
    width, pad = stand(1 + half), stand(5 + half)
    index = iota((MAXW, 1), 0)
    lane = iota((1, MAXW), 1)
    rate, inverse = rate_of(width), inverse_norm(width, pad)
    depth = jnp.where(half == 0, index, MAXW - 1.0 - index)
    need, best, _ = cover(width, pad, depth)
    place = slots(need, best)
    plain = wall_coeff(depth + lane + 1.0, rate, pad, inverse)
    plain = jnp.where((place < 0.0) & (lane < best), plain, 0.0)
    take = jnp.where(place == lane, 1.0, plain)
    outer = jnp.where(half == 0, where_ref[0] == 0, where_ref[0] == where_ref[1] - 1)
    take = jnp.where(outer, 0.0, take)
    ah_ref[0], al_ref[0] = split(take)
    apart = jnp.abs(iota((1, 2 * MAXW), 1) - (index + (half * MAXW).astype(jnp.float32)))
    hh_ref[...], hl_ref[...] = split(wall_coeff(apart, rate, pad, inverse))

    @pl.when(half == last)
    def _():
        uu, vv, ww, uv, uw, vw = (stress_ref[k : k + 1, :] for k in range(6))
        lund_aa = jnp.sqrt(uu)
        lund_ba = uv / lund_aa
        lund_bb = jnp.sqrt(vv - lund_ba * lund_ba)
        lund_ca = uw / lund_aa
        lund_cb = (vw - lund_ba * lund_ca) / lund_bb
        lund_cc = jnp.sqrt(ww - lund_ca * lund_ca - lund_cb * lund_cb)
        mean = stress_ref[6:7, :]
        lines = [lund_aa, lund_ba, lund_bb, lund_ca, lund_cb, lund_cc, mean, mean]
        lines.append(jnp.zeros((120, stress_ref.shape[1]), jnp.float32))
        lund_ref[...] = jnp.transpose(jnp.concatenate(lines, axis=0))


def late_tables(where, rows, stress_rows):
    rows_here = stress_rows.shape[1]
    take = jax.ShapeDtypeStruct((2, MAXW, MAXW), jnp.bfloat16)
    local = jax.ShapeDtypeStruct((rows_here, rows_here), jnp.bfloat16)
    take_block = pl.BlockSpec((1, MAXW, MAXW), lambda h: (h, 0, 0))
    local_block = pl.BlockSpec((MAXW, rows_here), lambda h: (h, 0))
    ah, al, hh, hl, lund = pl.pallas_call(
        late_kernel,
        grid=(2,),
        in_specs=[pl.BlockSpec(memory_space=pltpu.SMEM), whole(rows), whole(stress_rows)],
        out_specs=[take_block, take_block, local_block, local_block, pl.BlockSpec((rows_here, 128), lambda h: (0, 0))],
        out_shape=[take, take, local, local, jax.ShapeDtypeStruct((rows_here, 128), jnp.float32)],
        name="late",
    )(where, rows, stress_rows)
    return (ah, al), (hh, hl), lund


def widened(block):
    zero = jnp.zeros((REACH, REACH), block.dtype)
    left = jnp.concatenate([block, zero], axis=0)
    return jnp.concatenate([left, jnp.concatenate([zero, block], axis=0)], axis=1)


def span_block(square_ref, span):
    spread = jnp.full((1, 1), span, jnp.int32).astype(jnp.float32)
    rate = rate_of(spread)
    steps = iota((1, 4 * REACH), 1) - 2 * REACH
    profile = jnp.where(jnp.abs(steps) <= 2.0 * spread, jnp.exp(steps * steps * rate), 0.0)
    inverse = 1.0 / jnp.sqrt(jnp.sum(profile * profile, axis=1, keepdims=True))
    square = square_ref[...]
    return split(jnp.where(square <= 4.0 * spread * spread, jnp.exp(square * rate) * inverse, 0.0))


def front_kernel(build, cuts, spans, *refs):
    band = pl.program_id(0)
    if build:
        where_ref, span_ref, *refs = refs
        *refs, square_ref = refs
    x_ref, low_ref, high_ref, wh_ref, wl_ref, gh_ref, gl_ref = refs[:7]
    if build:
        refs = refs[7:]

        @pl.when(band == 0)
        def _():
            shift = iota((3 * REACH, REACH), 0) - REACH - iota((3 * REACH, REACH), 1)
            square_ref[...] = shift * shift

        block_high, block_low = span_block(square_ref, span_ref[where_ref[0] * pl.num_programs(0) + band])
        gh_ref[0], gl_ref[0] = block_high, block_low
    else:
        refs = refs[9:]
        block_high, block_low = gh_ref[0], gl_ref[0]
    sh_ref, sl_ref, *sends, keep_high, keep_low = refs
    per = MAXW // BAND
    tiles = x_ref.shape[2] // TILE
    wide = jnp.concatenate([low_ref[0], x_ref[0], high_ref[0]], axis=1)
    wide_high, wide_low = split(wide)
    x_high = jnp.concatenate([wide_high[:, t * TILE : (t + 2) * TILE] for t in range(tiles)], axis=0)
    x_low = jnp.concatenate([wide_low[:, t * TILE : (t + 2) * TILE] for t in range(tiles)], axis=0)
    high, low = split(dot3(x_high, x_low, widened(block_high), widened(block_low)))
    start = pl.multiple_of((band % per) * BAND, BAND)
    for t in range(tiles):
        cols = slice(t * TILE, (t + 1) * TILE)
        rows = slice(t * BAND, (t + 1) * BAND)
        sh_ref[0, :, cols] = high[rows]
        sl_ref[0, :, cols] = low[rows]
        keep_high[pl.ds(start, BAND), cols] = high[rows]
        keep_low[pl.ds(start, BAND), cols] = low[rows]

    for half in range(2):

        @pl.when(band == (per - 1 if half == 0 else pl.num_programs(0) - 1))
        def _(half=half):
            step = 2 * TILE
            width = x_ref.shape[2] // cuts
            for cut in range(cuts):
                refs_here = sends[2 * cut * len(spans) + half : 2 * (cut + 1) * len(spans) : 2]

                def body(t, carry, cut=cut, refs_here=refs_here):
                    here = pl.ds(pl.multiple_of(t * step, step), step)
                    cols = pl.ds(pl.multiple_of(t * step + cut * width, step), step)
                    value = dot3(wh_ref[0], wl_ref[0], keep_high[:, cols], keep_low[:, cols])
                    for (top, end), send_ref in zip(spans, refs_here):
                        send_ref[:, here] = value[top:end]
                    return carry

                lax.fori_loop(0, width // step, body, 0)


def front(spans, field, low, high, tables, give, held, channel, cuts, where=None, span_widths=None):
    channels, rows, cols = field.shape
    build = tables is None
    bands = rows // BAND
    width = cols // cuts
    size = spans[-1][1]
    pieces = [span for _ in range(cuts) for span in spans]
    halo = pl.BlockSpec((1, BAND, REACH), lambda b: (max(channel - 1, 0), b, 0))
    toeplitz = pl.BlockSpec((1, 3 * REACH, REACH), lambda b: (b, 0, 0))
    half = pl.BlockSpec((1, size, MAXW), lambda b: (b * 2 // bands, 0, 0))
    line = pl.BlockSpec((1, BAND, cols), lambda b: (channel, b, 0))
    in_specs = [line, halo, halo, half, half]
    operands = [field, low, high, *give]
    kept = jax.ShapeDtypeStruct((channels, rows, cols), jnp.bfloat16)
    sends = [jax.ShapeDtypeStruct((end - top, width), jnp.float32) for top, end in pieces for _ in range(2)]
    out_specs = [line, line] + [whole(send) for send in sends]
    out_shape = [kept, kept] + sends
    scratch = [pltpu.VMEM((MAXW, cols), jnp.bfloat16)] * 2
    aliases = {}
    if build:
        in_specs = [pl.BlockSpec(memory_space=pltpu.SMEM)] * 2 + in_specs
        operands = [where, span_widths] + operands
        out_specs = [toeplitz, toeplitz] + out_specs
        out_shape = [jax.ShapeDtypeStruct((bands, 3 * REACH, REACH), jnp.bfloat16)] * 2 + out_shape
        scratch = scratch + [pltpu.VMEM((3 * REACH, REACH), jnp.float32)]
    else:
        in_specs = in_specs + [toeplitz, toeplitz] + [pl.BlockSpec(memory_space=pl.ANY)] * 2
        operands = operands + [*tables, *held]
        aliases = {len(operands) - 2: 0, len(operands) - 1: 1}
    results = pl.pallas_call(
        functools.partial(front_kernel, build, cuts, spans),
        grid=(bands,),
        in_specs=in_specs,
        out_specs=out_specs,
        out_shape=out_shape,
        scratch_shapes=scratch,
        input_output_aliases=aliases,
        cost_estimate=pl.CostEstimate(
            flops=6 * rows * cols * 2 * TILE + 12 * size * MAXW * cols,
            bytes_accessed=rows * cols * 8 + size * cols * 8,
            transcendentals=0,
        ),
        name="front",
    )(*operands)
    if build:
        tables, results = results[:2], results[2:]
    outs = results[:2], [tuple(results[2 + 2 * k : 4 + 2 * k]) for k in range(len(pieces))]
    return (tables, *outs) if build else outs


def across(ah_ref, al_ref, half, recv):
    size = recv.shape[0]
    high, low = split(recv)
    return dot3(ah_ref[half, :, :size], al_ref[half, :, :size], high, low)


def main_kernel(counts, sh_ref, sl_ref, *rest):
    arrived = rest[: 2 * sum(counts)]
    ah_ref, al_ref, hh_ref, hl_ref, lund_ref, out_ref = rest[2 * sum(counts) :]

    def body(channel, carry):
        out_ref[channel] = dot3(hh_ref[...], hl_ref[...], sh_ref[channel], sl_ref[channel])
        return carry

    lax.fori_loop(0, sh_ref.shape[0], body, 0)

    def psi(channel):
        start = 2 * sum(counts[:channel])
        sums = []
        for half in range(2):
            parts = [ref[...] for ref in arrived[start + half : start + 2 * counts[channel] : 2]]
            sums.append(across(ah_ref, al_ref, half, jnp.concatenate(parts, axis=0)))
        return out_ref[channel] + jnp.concatenate(sums, axis=0)

    column = lambda k: lund_ref[:, k : k + 1]
    first, second = psi(0), out_ref[1]
    out_ref[0] = column(6) + column(0) * first
    out_ref[1] = column(1) * first + column(2) * second
    out_ref[2] = column(3) * first + column(4) * second + column(5) * out_ref[2]


ROOM = pltpu.CompilerParams(vmem_limit_bytes=56 * 1024 * 1024)


def main_filter(held, arrived, take, local, lund):
    channels, rows, cols = held[0].shape
    counts = tuple(len(pieces) for pieces in arrived)
    recv = [array for pieces in arrived for pair in pieces for array in pair]
    step = TILE
    block = pl.BlockSpec((channels, rows, step), lambda t: (0, 0, t))
    return pl.pallas_call(
        functools.partial(main_kernel, counts),
        grid=(cols // step,),
        in_specs=[block, block]
        + [pl.BlockSpec((array.shape[0], step), lambda t: (0, t)) for array in recv]
        + [whole(array) for array in (*take, *local, lund)],
        out_specs=block,
        out_shape=jax.ShapeDtypeStruct((channels, rows, cols), jnp.float32),
        compiler_params=ROOM,
        cost_estimate=pl.CostEstimate(
            flops=6 * channels * rows * rows * cols, bytes_accessed=channels * rows * cols * 8, transcendentals=0
        ),
        name="main",
    )(*held, *recv, *take, *local, lund)


def update_kernel(channel, top, bottom, ah_ref, al_ref, lund_ref, out_in_ref, out_ref, sum_ref):
    target = pl.program_id(1)
    column = channel * (channel + 3) // 2

    def body(t, carry):
        cols = pl.ds(pl.multiple_of(t * TILE, TILE), TILE)
        for half, recv in ((0, top), (1, bottom)):
            rows = slice(half * MAXW, (half + 1) * MAXW)
            value = across(ah_ref, al_ref, half, recv[:, cols])
            if channel == 1:
                sum_ref[rows, cols] = value
            out_ref[0, rows, cols] = out_in_ref[0, rows, cols] + lund_ref[rows, column : column + 1] * value
        return carry

    @pl.when(target == 0)
    def _():
        lax.fori_loop(0, out_ref.shape[2] // TILE, body, 0)

    if channel == 1:

        @pl.when(target == 1)
        def _():
            out_ref[0] = out_in_ref[0] + lund_ref[:, 4:5] * sum_ref[...]


def update(out, arrived, take, lund, channel, first):
    channels, rows, _ = out.shape
    size, width = arrived[0].shape
    step = min(4 * TILE if channel == 1 else 2 * TILE, width)
    block = pl.BlockSpec((1, rows, step), lambda t, k: (channel + k, 0, t + first // step))
    return pl.pallas_call(
        functools.partial(update_kernel, channel),
        grid=(width // step, channels - channel),
        in_specs=[pl.BlockSpec((size, step), lambda t, k: (0, t))] * 2
        + [whole(array) for array in (*take, lund)]
        + [block],
        out_specs=block,
        out_shape=jax.ShapeDtypeStruct(out.shape, out.dtype),
        scratch_shapes=[pltpu.VMEM((rows, step), jnp.float32)],
        input_output_aliases={5: 0},
        compiler_params=ROOM,
        cost_estimate=pl.CostEstimate(
            flops=6 * rows * size * width, bytes_accessed=rows * width * 8 + size * width * 8, transcendentals=0
        ),
        name="update",
    )(*arrived, *take, lund, out)


def ring(axis):
    count = lax.axis_size(axis)
    forward = [(i, (i + 1) % count) for i in range(count)]
    return forward, [(target, source) for source, target in forward]


def exchange(field):
    forward, backward = ring("span")
    low = lax.ppermute(field[:, :, -REACH:], "span", forward)
    return low, lax.ppermute(field[:, :, :REACH], "span", backward)


def shards(random_field, half_widths, band_pads, span_widths, stresses, mean_flow):
    _, _, cols = random_field.shape
    wall_count = lax.axis_size("wall")
    where = jnp.stack([lax.axis_index("wall"), jnp.int32(wall_count)])
    halo = exchange(random_field[:1])
    give, rows, needed = early_tables(where, band_pads, half_widths)
    rest, needed = lax.optimization_barrier((random_field, needed))
    halos = exchange(rest[1:])
    downward, upward = ring("wall")
    spans = list(zip((0,) + SIZES[:-1], SIZES))
    tables, held, ahead = front(spans, random_field, *halo, None, give, None, 0, 1, where, span_widths)

    def across_edges(pieces):
        arrived = []
        for up, down in pieces:
            bottom = lax.ppermute(up, "wall", upward)
            arrived.append((lax.ppermute(down, "wall", downward), bottom))
        return arrived

    def run(number, *operands):
        return steps(number, *operands)

    def steps(number, field, halos, tables, give, where, rows, stresses, mean_flow, held, ahead):
        span = [(0, SIZES[number])]
        first = across_edges(ahead[: number + 1])
        held, pieces = front(span, field, *halos, tables, give, held, 1, 1)
        second = across_edges(pieces)
        held, pieces = front(span, field, *halos, tables, give, held, 2, 2)
        third = across_edges(pieces[:1]) + across_edges(pieces[1:])
        stress_rows = jnp.pad(jnp.concatenate([stresses, mean_flow[None]], axis=0), ((0, 1), (0, 0)))
        take, local, lund = late_tables(where, rows, stress_rows)
        out = main_filter(held, (first,), take, local, lund)
        out = update(out, second[0], take, lund, 1, 0)
        for k, pair in enumerate(third):
            out = update(out, pair, take, lund, 2, k * (cols // len(third)))
        return out

    operands = (random_field, halos, tables, give, where, rows, stresses, mean_flow, held, ahead)
    if len(SIZES) == 1:
        return run(0, *operands)
    which = sum((needed > size).astype(jnp.int32) for size in SIZES[:-1])
    return lax.switch(which, [functools.partial(run, k) for k in range(len(SIZES))], *operands)


def solution(mesh):
    return jax.shard_map(
        shards,
        mesh=mesh,
        in_specs=(P(None, "wall", "span"), P(), P(), P(), P(None, "wall"), P("wall")),
        out_specs=P(None, "wall", "span"),
        check_vma=False,
    )
```

```python
import functools

import jax
import jax.numpy as jnp
from jax import lax
from jax.experimental import pallas as pl
from jax.experimental.pallas import tpu as pltpu
from jax.sharding import PartitionSpec as P

MAXW = 256
SPMAX = 64
BAND = 64
REACH = 2 * SPMAX
PER_STEP = 2
ROOM = pltpu.CompilerParams(vmem_limit_bytes=64 * 1024 * 1024)
TILE = 4 * SPMAX
SIZES = (152, 184, 256)


def split(values):
    high = values.astype(jnp.bfloat16)
    return high, (values - high.astype(jnp.float32)).astype(jnp.bfloat16)


def dot(left, right):
    return lax.dot_general(left, right, (((1,), (0,)), ((), ())), preferred_element_type=jnp.float32)


def dot3(left_high, left_low, right_high, right_low):
    return dot(left_high, right_high) + (dot(left_high, right_low) + dot(left_low, right_high))


def whole(array):
    return pl.BlockSpec(array.shape, lambda *_: (0,) * len(array.shape))


def iota(shape, axis):
    return lax.broadcasted_iota(jnp.int32, shape, axis).astype(jnp.float32)


def wall_coeff(distance, rate, pad, inverse):
    return jnp.where(distance <= pad, jnp.exp(distance * distance * rate) * inverse, 0.0)


def rate_of(width):
    return (-0.5 * jnp.pi) / (width * width)


def inverse_norm(width, pad):
    steps = iota((1, MAXW + 128), 1)
    profile = wall_coeff(steps, rate_of(width), pad, 1.0)
    return 1.0 / jnp.sqrt(2.0 * jnp.sum(profile * profile, axis=1, keepdims=True) - 1.0)


def cover(width, pad, depth):
    need = jnp.floor(jnp.minimum(pad, width * 8.25)) - depth
    counts = iota((1, MAXW + 128), 1)
    total = jnp.sum(jnp.where(need > counts, 1.0, 0.0), axis=0, keepdims=True) + counts
    key = jnp.min(jnp.where(counts <= MAXW, total, 4096.0) * 512.0 + counts, axis=1, keepdims=True)
    cost = jnp.floor(key * (1.0 / 512.0))
    best = key - cost * 512.0
    return need, best, cost


def slots(need, best):
    part = jnp.where(need > best, 1.0, 0.0)
    earlier = jnp.where(iota((MAXW, MAXW), 1) < iota((MAXW, MAXW), 0), 1.0, 0.0).astype(jnp.bfloat16)
    before = dot(earlier, jnp.broadcast_to(part, (MAXW, 128)).astype(jnp.bfloat16))[:, :1]
    return jnp.where(part > 0.0, best + before, -1.0)


def early_kernel(
    segments, where_ref, pads_ref, widths_ref, wh_ref, wl_ref, rows_ref, needed_ref, plane_ref
):
    where = where_ref[0]
    per = MAXW // BAND

    plane_ref[...] = jnp.ones(plane_ref.shape, jnp.float32)
    widths = widths_ref[...].astype(jnp.float32)
    split_by = MAXW // widths.shape[1]
    lanes = lax.broadcasted_iota(jnp.int32, (1, MAXW), 1)
    for segment in range(segments):
        parts = [widths[segment * split_by + k : segment * split_by + k + 1] for k in range(split_by)]
        plane_ref[0, segment + 1 : segment + 2, :] = jnp.concatenate(parts, axis=1)
        line = jnp.full((1, MAXW), pads_ref[segment * per], jnp.int32)
        for k in range(1, per):
            line = jnp.where(lanes >= k * BAND, pads_ref[segment * per + k], line)
        plane_ref[1, segment + 1 : segment + 2, :] = line.astype(jnp.float32)
    rows_ref[...] = jnp.ones(rows_ref.shape, jnp.float32)
    for k in range(2):
        for j in range(4):
            rows_ref[4 * k + j : 4 * k + j + 1, :] = plane_ref[k, pl.ds(2 * where + j, 1), :]
        rows_ref[8 + k * segments : 8 + (k + 1) * segments, :] = plane_ref[k, 1 : segments + 1, :]
    columns = jnp.transpose(rows_ref[...])
    column = lambda k: columns[:, k : k + 1]
    index = iota((MAXW, 1), 0)
    lane = iota((1, MAXW), 1)

    for half, segment in ((0, 0), (1, 3)):
        width, pad = column(segment), column(4 + segment)
        depth = MAXW - 1.0 - index if half == 0 else index
        away = lane + 1.0 if half == 0 else MAXW - lane
        need, best, _ = cover(width, pad, depth)
        place = slots(need, best)
        chosen = jnp.where(place == lane, 1.0, 0.0).astype(jnp.bfloat16)
        high, low = split(wall_coeff(depth + away, rate_of(width), pad, inverse_norm(width, pad)))
        pick = lambda values: lax.dot_general(
            chosen, values, (((0,), (0,)), ((), ())), preferred_element_type=jnp.float32
        )
        plain = jnp.where((away == index + 1.0) & (index < best), 1.0, 0.0)
        wh_ref[half] = (pick(high) + plain).astype(jnp.bfloat16)
        wl_ref[half] = pick(low).astype(jnp.bfloat16)

    most = jnp.zeros((1, 1), jnp.float32)
    for segment in range(1, segments - 1):
        depth = MAXW - 1.0 - index if segment % 2 else index
        cost = cover(column(8 + segment), column(8 + segments + segment), depth)[2]
        most = jnp.maximum(most, cost)
    needed_ref[0, 0] = jnp.max(most).astype(jnp.int32)


def early_tables(where, band_pads, half_widths):
    segments = half_widths.shape[0] // MAXW
    half_widths = half_widths.reshape(-1, 128)
    give = jax.ShapeDtypeStruct((2, MAXW, MAXW), jnp.bfloat16)
    rows = jax.ShapeDtypeStruct((128, MAXW), jnp.float32)
    smem = pl.BlockSpec(memory_space=pltpu.SMEM)
    vmem = pl.BlockSpec(memory_space=pltpu.VMEM)
    wh, wl, rows, needed = pl.pallas_call(
        functools.partial(early_kernel, segments),
        in_specs=[smem, smem, vmem],
        out_specs=[vmem, vmem, vmem, smem],
        out_shape=[give, give, rows, jax.ShapeDtypeStruct((1, 1), jnp.int32)],
        scratch_shapes=[pltpu.VMEM((2, segments + 8, MAXW), jnp.float32)],
        name="early",
    )(where, band_pads, half_widths)
    return (wh, wl), rows, needed[0, 0]


def late_kernel(where_ref, rows_ref, stress_ref, ah_ref, al_ref, hh_ref, hl_ref, lund_ref):
    half = pl.program_id(0)
    last = pl.num_programs(0) - 1
    stand = lambda k: jnp.transpose(jnp.broadcast_to(rows_ref[pl.ds(k, 1), :], (128, MAXW)))[:, :1]
    width, pad = stand(1 + half), stand(5 + half)
    index = iota((MAXW, 1), 0)
    lane = iota((1, MAXW), 1)
    rate, inverse = rate_of(width), inverse_norm(width, pad)
    depth = jnp.where(half == 0, index, MAXW - 1.0 - index)
    need, best, _ = cover(width, pad, depth)
    place = slots(need, best)
    plain = wall_coeff(depth + lane + 1.0, rate, pad, inverse)
    plain = jnp.where((place < 0.0) & (lane < best), plain, 0.0)
    take = jnp.where(place == lane, 1.0, plain)
    outer = jnp.where(half == 0, where_ref[0] == 0, where_ref[0] == where_ref[1] - 1)
    take = jnp.where(outer, 0.0, take)
    ah_ref[0], al_ref[0] = split(take)
    apart = jnp.abs(iota((1, 2 * MAXW), 1) - (index + (half * MAXW).astype(jnp.float32)))
    hh_ref[...], hl_ref[...] = split(wall_coeff(apart, rate, pad, inverse))

    @pl.when(half == last)
    def _():
        uu, vv, ww, uv, uw, vw = (stress_ref[k : k + 1, :] for k in range(6))
        lund_aa = jnp.sqrt(uu)
        lund_ba = uv / lund_aa
        lund_bb = jnp.sqrt(vv - lund_ba * lund_ba)
        lund_ca = uw / lund_aa
        lund_cb = (vw - lund_ba * lund_ca) / lund_bb
        lund_cc = jnp.sqrt(ww - lund_ca * lund_ca - lund_cb * lund_cb)
        mean = stress_ref[6:7, :]
        lines = [lund_aa, lund_ba, lund_bb, lund_ca, lund_cb, lund_cc, mean, mean]
        lines.append(jnp.zeros((120, stress_ref.shape[1]), jnp.float32))
        lund_ref[...] = jnp.transpose(jnp.concatenate(lines, axis=0))


def late_tables(where, rows, stress_rows):
    rows_here = stress_rows.shape[1]
    take = jax.ShapeDtypeStruct((2, MAXW, MAXW), jnp.bfloat16)
    local = jax.ShapeDtypeStruct((rows_here, rows_here), jnp.bfloat16)
    take_block = pl.BlockSpec((1, MAXW, MAXW), lambda h: (h, 0, 0))
    local_block = pl.BlockSpec((MAXW, rows_here), lambda h: (h, 0))
    ah, al, hh, hl, lund = pl.pallas_call(
        late_kernel,
        grid=(2,),
        in_specs=[pl.BlockSpec(memory_space=pltpu.SMEM), whole(rows), whole(stress_rows)],
        out_specs=[take_block, take_block, local_block, local_block, pl.BlockSpec((rows_here, 128), lambda h: (0, 0))],
        out_shape=[take, take, local, local, jax.ShapeDtypeStruct((rows_here, 128), jnp.float32)],
        compiler_params=ROOM,
        name="late",
    )(where, rows, stress_rows)
    return (ah, al), (hh, hl), lund


def widened(block):
    zero = jnp.zeros((REACH, REACH), block.dtype)
    left = jnp.concatenate([block, zero], axis=0)
    return jnp.concatenate([left, jnp.concatenate([zero, block], axis=0)], axis=1)


def span_block(square_ref, span):
    spread = jnp.full((1, 1), span, jnp.int32).astype(jnp.float32)
    rate = rate_of(spread)
    steps = iota((1, 4 * REACH), 1) - 2 * REACH
    profile = jnp.where(jnp.abs(steps) <= 2.0 * spread, jnp.exp(steps * steps * rate), 0.0)
    inverse = 1.0 / jnp.sqrt(jnp.sum(profile * profile, axis=1, keepdims=True))
    square = square_ref[...]
    return split(jnp.where(square <= 4.0 * spread * spread, jnp.exp(square * rate) * inverse, 0.0))


def front_kernel(build, cuts, spans, *refs):
    step_id = pl.program_id(0)
    if build:
        where_ref, span_ref, *refs = refs
        *refs, square_ref = refs
    x_ref, low_ref, high_ref, wh_ref, wl_ref, gh_ref, gl_ref = refs[:7]
    if build:
        refs = refs[7:]

        @pl.when(step_id == 0)
        def _():
            shift = iota((3 * REACH, REACH), 0) - REACH - iota((3 * REACH, REACH), 1)
            square_ref[...] = shift * shift

    else:
        refs = refs[9:]
    sh_ref, sl_ref, *sends, keep_high, keep_low = refs
    per = MAXW // BAND
    tiles = x_ref.shape[2] // TILE

    def filter_band(k, carry):
        band = step_id * PER_STEP + k
        here = pl.ds(pl.multiple_of(k * BAND, BAND), BAND)
        if build:
            bands = pl.num_programs(0) * PER_STEP
            block_high, block_low = span_block(square_ref, span_ref[where_ref[0] * bands + band])
            gh_ref[k], gl_ref[k] = block_high, block_low
        else:
            block_high, block_low = gh_ref[k], gl_ref[k]
        wide = jnp.concatenate([low_ref[0, here, :], x_ref[0, here, :], high_ref[0, here, :]], axis=1)
        wide_high, wide_low = split(wide)
        x_high = jnp.concatenate([wide_high[:, t * TILE : (t + 2) * TILE] for t in range(tiles)], axis=0)
        x_low = jnp.concatenate([wide_low[:, t * TILE : (t + 2) * TILE] for t in range(tiles)], axis=0)
        high, low = split(dot3(x_high, x_low, widened(block_high), widened(block_low)))
        kept = pl.ds(pl.multiple_of((band % per) * BAND, BAND), BAND)
        for t in range(tiles):
            cols = slice(t * TILE, (t + 1) * TILE)
            rows = slice(t * BAND, (t + 1) * BAND)
            sh_ref[0, here, cols] = high[rows]
            sl_ref[0, here, cols] = low[rows]
            keep_high[kept, cols] = high[rows]
            keep_low[kept, cols] = low[rows]
        return carry

    lax.fori_loop(0, PER_STEP, filter_band, 0)

    for half in range(2):

        @pl.when(step_id == (per // PER_STEP - 1 if half == 0 else pl.num_programs(0) - 1))
        def _(half=half):
            step = 2 * TILE
            width = x_ref.shape[2] // cuts
            for cut in range(cuts):
                refs_here = sends[2 * cut * len(spans) + half : 2 * (cut + 1) * len(spans) : 2]

                def body(t, carry, cut=cut, refs_here=refs_here):
                    here = pl.ds(pl.multiple_of(t * step, step), step)
                    cols = pl.ds(pl.multiple_of(t * step + cut * width, step), step)
                    value = dot3(wh_ref[0], wl_ref[0], keep_high[:, cols], keep_low[:, cols])
                    for (top, end), send_ref in zip(spans, refs_here):
                        send_ref[:, here] = value[top:end]
                    return carry

                lax.fori_loop(0, width // step, body, 0)


def front(spans, field, low, high, tables, give, held, channel, cuts, where=None, span_widths=None):
    channels, rows, cols = field.shape
    build = tables is None
    bands = rows // BAND
    width = cols // cuts
    size = spans[-1][1]
    pieces = [span for _ in range(cuts) for span in spans]
    step_rows = PER_STEP * BAND
    halo = pl.BlockSpec((1, step_rows, REACH), lambda b: (max(channel - 1, 0), b, 0))
    toeplitz = pl.BlockSpec((PER_STEP, 3 * REACH, REACH), lambda b: (b, 0, 0))
    half = pl.BlockSpec((1, size, MAXW), lambda b: (b * 2 * PER_STEP // bands, 0, 0))
    line = pl.BlockSpec((1, step_rows, cols), lambda b: (channel, b, 0))
    in_specs = [line, halo, halo, half, half]
    operands = [field, low, high, *give]
    kept = jax.ShapeDtypeStruct((channels, rows, cols), jnp.bfloat16)
    sends = [jax.ShapeDtypeStruct((end - top, width), jnp.float32) for top, end in pieces for _ in range(2)]
    out_specs = [line, line] + [whole(send) for send in sends]
    out_shape = [kept, kept] + sends
    scratch = [pltpu.VMEM((MAXW, cols), jnp.bfloat16)] * 2
    aliases = {}
    if build:
        in_specs = [pl.BlockSpec(memory_space=pltpu.SMEM)] * 2 + in_specs
        operands = [where, span_widths] + operands
        out_specs = [toeplitz, toeplitz] + out_specs
        out_shape = [jax.ShapeDtypeStruct((bands, 3 * REACH, REACH), jnp.bfloat16)] * 2 + out_shape
        scratch = scratch + [pltpu.VMEM((3 * REACH, REACH), jnp.float32)]
    else:
        in_specs = in_specs + [toeplitz, toeplitz] + [pl.BlockSpec(memory_space=pl.ANY)] * 2
        operands = operands + [*tables, *held]
        aliases = {len(operands) - 2: 0, len(operands) - 1: 1}
    results = pl.pallas_call(
        functools.partial(front_kernel, build, cuts, spans),
        grid=(bands // PER_STEP,),
        in_specs=in_specs,
        out_specs=out_specs,
        out_shape=out_shape,
        scratch_shapes=scratch,
        input_output_aliases=aliases,
        cost_estimate=pl.CostEstimate(
            flops=6 * rows * cols * 2 * TILE + 12 * size * MAXW * cols,
            bytes_accessed=rows * cols * 8 + size * cols * 8,
            transcendentals=0,
        ),
        compiler_params=None if build else ROOM,
        name="front",
    )(*operands)
    if build:
        tables, results = results[:2], results[2:]
    outs = results[:2], [tuple(results[2 + 2 * k : 4 + 2 * k]) for k in range(len(pieces))]
    return (tables, *outs) if build else outs


def across(ah_ref, al_ref, half, recv):
    size = recv.shape[0]
    high, low = split(recv)
    return dot3(ah_ref[half, :, :size], al_ref[half, :, :size], high, low)


def main_kernel(counts, sh_ref, sl_ref, *rest):
    arrived = rest[: 2 * sum(counts)]
    ah_ref, al_ref, hh_ref, hl_ref, lund_ref, out_ref = rest[2 * sum(counts) :]

    def psi(channel):
        value = dot3(hh_ref[...], hl_ref[...], sh_ref[channel], sl_ref[channel])
        if channel:
            return value
        sums = []
        for half in range(2):
            parts = [ref[...] for ref in arrived[half::2]]
            sums.append(across(ah_ref, al_ref, half, jnp.concatenate(parts, axis=0)))
        return value + jnp.concatenate(sums, axis=0)

    column = lambda k: lund_ref[:, k : k + 1]
    first = psi(0)
    out_ref[0] = column(6) + column(0) * first
    normal, spanwise = column(1) * first, column(3) * first
    second = psi(1)
    out_ref[1] = normal + column(2) * second
    out_ref[2] = spanwise + column(4) * second + column(5) * psi(2)


def main_filter(held, arrived, take, local, lund):
    channels, rows, cols = held[0].shape
    counts = tuple(len(pieces) for pieces in arrived)
    recv = [array for pieces in arrived for pair in pieces for array in pair]
    step = TILE
    block = pl.BlockSpec((channels, rows, step), lambda t: (0, 0, t))
    return pl.pallas_call(
        functools.partial(main_kernel, counts),
        grid=(cols // step,),
        in_specs=[block, block]
        + [pl.BlockSpec((array.shape[0], step), lambda t: (0, t)) for array in recv]
        + [whole(array) for array in (*take, *local, lund)],
        out_specs=block,
        out_shape=jax.ShapeDtypeStruct((channels, rows, cols), jnp.float32),
        compiler_params=ROOM,
        cost_estimate=pl.CostEstimate(
            flops=6 * channels * rows * rows * cols, bytes_accessed=channels * rows * cols * 8, transcendentals=0
        ),
        name="main",
    )(*held, *recv, *take, *local, lund)


def update_kernel(channel, top, bottom, ah_ref, al_ref, lund_ref, out_in_ref, out_ref, sum_ref):
    target = pl.program_id(1)
    column = channel * (channel + 3) // 2

    def body(t, carry):
        cols = pl.ds(pl.multiple_of(t * TILE, TILE), TILE)
        for half, recv in ((0, top), (1, bottom)):
            rows = slice(half * MAXW, (half + 1) * MAXW)
            value = across(ah_ref, al_ref, half, recv[:, cols])
            if channel == 1:
                sum_ref[rows, cols] = value
            out_ref[0, rows, cols] = out_in_ref[0, rows, cols] + lund_ref[rows, column : column + 1] * value
        return carry

    @pl.when(target == 0)
    def _():
        lax.fori_loop(0, out_ref.shape[2] // TILE, body, 0)

    if channel == 1:

        @pl.when(target == 1)
        def _():
            out_ref[0] = out_in_ref[0] + lund_ref[:, 4:5] * sum_ref[...]


def update(out, arrived, take, lund, channel, first):
    channels, rows, _ = out.shape
    size, width = arrived[0].shape
    step = min(4 * TILE if channel == 1 else 2 * TILE, width)
    block = pl.BlockSpec((1, rows, step), lambda t, k: (channel + k, 0, t + first // step))
    return pl.pallas_call(
        functools.partial(update_kernel, channel),
        grid=(width // step, channels - channel),
        in_specs=[pl.BlockSpec((size, step), lambda t, k: (0, t))] * 2
        + [whole(array) for array in (*take, lund)]
        + [block],
        out_specs=block,
        out_shape=jax.ShapeDtypeStruct(out.shape, out.dtype),
        scratch_shapes=[pltpu.VMEM((rows, step), jnp.float32)],
        input_output_aliases={5: 0},
        compiler_params=ROOM,
        cost_estimate=pl.CostEstimate(
            flops=6 * rows * size * width, bytes_accessed=rows * width * 8 + size * width * 8, transcendentals=0
        ),
        name="update",
    )(*arrived, *take, lund, out)


def ring(axis):
    count = lax.axis_size(axis)
    forward = [(i, (i + 1) % count) for i in range(count)]
    return forward, [(target, source) for source, target in forward]


def exchange(field):
    forward, backward = ring("span")
    low = lax.ppermute(field[:, :, -REACH:], "span", forward)
    return low, lax.ppermute(field[:, :, :REACH], "span", backward)


def shards(random_field, half_widths, band_pads, span_widths, stresses, mean_flow):
    _, _, cols = random_field.shape
    wall_count = lax.axis_size("wall")
    where = jnp.stack([lax.axis_index("wall"), jnp.int32(wall_count)])
    halo = exchange(random_field[:1])
    give, rows, needed = early_tables(where, band_pads, half_widths)
    downward, upward = ring("wall")
    spans = list(zip((0,) + SIZES[:-1], SIZES))
    tables, held, ahead = front(spans, random_field, *halo, None, give, None, 0, 1, where, span_widths)

    def across_edges(pieces):
        arrived = []
        for up, down in pieces:
            bottom = lax.ppermute(up, "wall", upward)
            arrived.append((lax.ppermute(down, "wall", downward), bottom))
        return arrived

    def run(number, *operands):
        return steps(number, *operands)

    def steps(number, field, tables, give, where, rows, stresses, mean_flow, held, ahead):
        span = [(0, SIZES[number])]
        first = across_edges(ahead[: number + 1])
        halos = exchange(field[1:])
        stress_rows = jnp.pad(jnp.concatenate([stresses, mean_flow[None]], axis=0), ((0, 1), (0, 0)))
        take, local, lund = late_tables(where, rows, stress_rows)
        held, pieces = front(span, field, *halos, tables, give, held, 1, 1)
        second = across_edges(pieces)
        held, pieces = front(span, field, *halos, tables, give, held, 2, 2)
        third = across_edges(pieces[:1]) + across_edges(pieces[1:])
        out = main_filter(held, (first,), take, local, lund)
        out = update(out, second[0], take, lund, 1, 0)
        for k, pair in enumerate(third):
            out = update(out, pair, take, lund, 2, k * (cols // len(third)))
        return out

    operands = (random_field, tables, give, where, rows, stresses, mean_flow, held, ahead)
    if len(SIZES) == 1:
        return run(0, *operands)
    which = sum((needed > size).astype(jnp.int32) for size in SIZES[:-1])
    return lax.switch(which, [functools.partial(run, k) for k in range(len(SIZES))], *operands)


def solution(mesh):
    return jax.shard_map(
        shards,
        mesh=mesh,
        in_specs=(P(None, "wall", "span"), P(), P(), P(), P(None, "wall"), P("wall")),
        out_specs=P(None, "wall", "span"),
        check_vma=False,
    )
```
